32 devices in a mesh: grp: 2 (over x), row: 4 (over y, core), diag: 4 (over z).
Axes of the slice: x: 2, y: 2, z: 4, core: 2. Of those that a mesh axis runs over, the one named last changes fastest.
Arguments:
- emb_rows: bfloat16 [32, 1024], P(None, ('grp', 'row')), parts along dimension 1, may hold values from -6 to 6
- emb_cols: bfloat16 [32, 1024], P(None, ('grp', 'row')), parts along dimension 1, may hold values from -6 to 6
- kernel: bfloat16 [3, 3, 32, 32], replicated, may hold values from -0.375 to 0.375
- bias: float32 [32], replicated, may hold values from -3 to 3
- cotangent: bfloat16 [32, 1024, 512], P(None, ('grp', 'row'), 'diag'), parts along dimension 1, may hold values from -6 to 6
- valid: int32 [1024], P(('grp', 'row')), parts along dimension 0, may hold values 0 or 1
- dilation: int32 [2], P('grp'), parts along dimension 0, may hold values from 1 to 4
- band: int32 [2], P('grp'), parts along dimension 0, may hold values from 384 to 512
Outputs:
- pair_out: bfloat16 [32, 1024, 512], P(None, ('grp', 'row'), 'diag'), parts along dimension 1
- row_grad: float32 [32, 1024], P(None, ('grp', 'row')), parts along dimension 1
- col_grad: float32 [32, 1024], P(None, ('grp', 'row')), parts along dimension 1
- kernel_grad: float32 [6, 3, 32, 32], P('grp'), parts along dimension 0
- bias_grad: float32 [64], P('grp'), parts along dimension 0
The draws below stay inside these ranges and needn't reach their ends.
There are 2 independent parts, one for each index of `grp`. The reference program is written for one: setup_inputs(seed, part) draws one part's arguments, and reference() takes and returns one part's arrays. A program takes and returns all parts, laid end to end along the dimension named above; an argument that names none is the same for every part. Nothing has to cross between parts.
All inputs are finite; a program needn't handle non-finite values. No bound on the sum of `valid` on one device may be relied on, other than what follows from the above.
Results may differ from the reference program's by a relative error of at most 0.0032.
Values may be sent and summed in bfloat16 or wider, within the bound.
A program may use at most 128 MiB of HBM per device.

```python
import jax
import jax.numpy as jnp
from jax import lax

CH = 32
MAXDIL = 4
ROWS_DEV = 128
LENGTH = 512
DIAGONAL_COUNT = 512


def touch_ends(drawn, stream_key, low, high):
    spot = [jax.random.randint(jax.random.fold_in(stream_key, axis), (), 0, length) for axis, length in enumerate(drawn.shape)]
    widest = drawn.shape.index(max(drawn.shape))
    neighbour = spot[:widest] + [(spot[widest] + 1) % drawn.shape[widest]] + spot[widest + 1:]
    return drawn.at[tuple(spot)].set(low).at[tuple(neighbour)].set(high)


def steps_of(rng, extent, cuts, low, top_value):
    level, own = 1.0, jax.random.fold_in(rng, 6)
    for dim, shards_of in cuts:
        draws = jnp.exp(jax.random.uniform(jax.random.fold_in(own, dim), (shards_of,), jnp.float32, low / len(cuts), top_value / len(cuts)))
        level = level * jnp.repeat(draws, extent[dim] // shards_of).reshape([-1 if axis == dim else 1 for axis in range(len(extent))])
    return level


def scatter_about(own_key, extent, deviation, limit, split=(), held_as=jnp.bfloat16):
    values = jax.random.normal(own_key, extent, jnp.float32) * deviation
    if len(split) > 0:
        values = steps_of(own_key, extent, split, -0.22, 0.18) * values
    return jnp.clip(values, min=-limit, max=limit).astype(held_as)


def setup_inputs(seed: int = 0, part: int = 0) -> dict:
    arg_keys = jax.random.split(jax.random.key(seed), 9)
    own_keys = jax.random.split(jax.random.fold_in(arg_keys[8], part), 9)
    return {
        "emb_rows": scatter_about(own_keys[0], (CH, LENGTH), 1.0, 6.0, ((1, 4),)),
        "emb_cols": scatter_about(own_keys[1], (CH, LENGTH), 1.0, 6.0, ((1, 4),)),
        "kernel": scatter_about(arg_keys[2], (3, 3, CH, CH), (9 * CH) ** -0.5, 0.375),
        "bias": scatter_about(arg_keys[3], (CH,), 0.5, 3.0, (), jnp.float32),
        "cotangent": scatter_about(own_keys[4], (CH, LENGTH, DIAGONAL_COUNT), 1.0, 6.0, ((1, 4), (2, 4))),
        "valid": touch_ends((jax.random.randint(own_keys[5], (LENGTH,), 0, 10) < 9).astype(jnp.int32), jax.random.fold_in(own_keys[5], 1), 0, 1),
        "dilation": jax.random.randint(own_keys[6], (1,), 1, MAXDIL + 1).astype(jnp.int32),
        "band": jax.random.randint(own_keys[7], (1,), DIAGONAL_COUNT * 3 // 4, DIAGONAL_COUNT + 1).astype(jnp.int32),
    }


def diagonal_take(window, row_number, diagonal_number):
    span_width = row_number + diagonal_number - 1
    leading = window.shape[:-1]
    widened = jnp.broadcast_to(window[..., None, :], leading + (row_number, span_width))
    flattened = widened.reshape(leading + (row_number * span_width,))
    flattened = jnp.pad(flattened, [(0, 0)] * len(leading) + [(0, row_number)])
    return flattened.reshape(leading + (row_number, span_width + 1))[..., :diagonal_number]

def diagonal_fold(field):
    channels, row_number, diagonal_number = field.shape
    span_width = row_number + diagonal_number - 1
    padded = jnp.pad(field, ((0, 0), (0, 0), (0, span_width + 1 - diagonal_number)))
    flattened = padded.reshape(channels, row_number * (span_width + 1))[:, :row_number * span_width]
    return lax.optimization_barrier(jnp.sum(flattened.reshape(channels, row_number, span_width), axis=1))

def diagonal_sums(field):
    channels, row_number, diagonal_number = field.shape
    block_row_list = 128 if row_number % 128 == 0 else row_number
    part_width = block_row_list + diagonal_number - 1

    def accumulate(index, totals):
        first = index * block_row_list
        piece = lax.dynamic_slice_in_dim(field, first, block_row_list, 1)
        current = lax.dynamic_slice_in_dim(totals, first, part_width, 1)
        return lax.dynamic_update_slice_in_dim(totals, current + diagonal_fold(piece), first, 1)
    totals = jnp.zeros((channels, row_number + diagonal_number - 1), jnp.float32)
    return lax.fori_loop(0, row_number // block_row_list, accumulate, totals)

def pair_block(row_embed, row_valid, col_window, col_valid, first_diag, row_number, diagonal_number, band_limit):
    outer = row_embed.astype(jnp.float32)[:, :, None] + diagonal_take(col_window, row_number, diagonal_number).astype(jnp.float32)
    offsets = first_diag + jnp.arange(diagonal_number, dtype=jnp.int32)
    inside = ((offsets >= 0) & (offsets < band_limit)).astype(jnp.float32)
    validity = row_valid[:, None] * diagonal_take(col_valid[None], row_number, diagonal_number)[0] * inside[None, :]
    hidden = outer * validity
    active = (jax.nn.gelu(hidden) * validity).astype(jnp.bfloat16)
    return (hidden, validity, active)

def contract(form, left, right):
    return jnp.einsum(form, left.astype(jnp.float32), right.astype(jnp.float32))

def dilated_convolve(active_extended, kernel, dilation_factor, row_number, diagonal_number, border_width):
    channels = active_extended.shape[0]
    result = jnp.zeros((kernel.shape[2], row_number, diagonal_number), jnp.float32)
    for kernel_tap_row in range(3):
        for kernel_tap_column in range(3):
            corner_patch = (jnp.int32(0), border_width + (kernel_tap_row - 1) * dilation_factor, border_width + (kernel_tap_column - kernel_tap_row) * dilation_factor)
            piece = lax.dynamic_slice(active_extended, corner_patch, (channels, row_number, diagonal_number))
            result = result + contract('oc,crk->ork', kernel[kernel_tap_row, kernel_tap_column], piece)
    return result

def kernel_summands(gradient_local, active_extended, dilation_factor, row_number, diagonal_number, border_width):
    channels = active_extended.shape[0]
    taps = []
    for kernel_tap_row in range(3):
        for kernel_tap_column in range(3):
            corner_patch = (jnp.int32(0), border_width + (kernel_tap_row - 1) * dilation_factor, border_width + (kernel_tap_column - kernel_tap_row) * dilation_factor)
            piece = lax.dynamic_slice(active_extended, corner_patch, (channels, row_number, diagonal_number))
            taps.append(contract('ork,crk->oc', gradient_local, piece))
    return jnp.stack(taps).reshape(3, 3, channels, channels)

def dilated_convolve_grad(gradient_extended, kernel, dilation_factor, row_number, diagonal_number, border_width):
    channels = gradient_extended.shape[0]
    result = jnp.zeros((kernel.shape[3], row_number, diagonal_number), jnp.float32)
    for kernel_tap_row in range(3):
        for kernel_tap_column in range(3):
            corner_patch = (jnp.int32(0), border_width - (kernel_tap_row - 1) * dilation_factor, border_width - (kernel_tap_column - kernel_tap_row) * dilation_factor)
            piece = lax.dynamic_slice(gradient_extended, corner_patch, (channels, row_number, diagonal_number))
            result = result + contract('oc,ork->crk', kernel[kernel_tap_row, kernel_tap_column], piece)
    return result

def reference(emb_rows, emb_cols, kernel, bias, cotangent, valid, dilation, band):
    border_width = 2 * MAXDIL
    block_row_list = ROWS_DEV
    channels = emb_rows.shape[0]
    dilation_factor = dilation[0]
    band_limit = band[0]
    valid_float = valid.astype(jnp.float32)
    cols_padded = jnp.pad(emb_cols, ((0, 0), (2 * border_width, DIAGONAL_COUNT + 2 * border_width + block_row_list)))
    cvalid_padded = jnp.pad(valid_float, (2 * border_width, DIAGONAL_COUNT + 2 * border_width + block_row_list))
    rows_padded = jnp.pad(emb_rows, ((0, 0), (border_width, border_width)))
    rvalid_padded = jnp.pad(valid_float, (border_width, border_width))
    grad_padded = jnp.pad(cotangent, ((0, 0), (border_width, border_width), (border_width, border_width)))

    def advance(carry, block_index):
        col_totals, kernel_total, bias_total = carry
        first = block_index * block_row_list
        row_embed = lax.dynamic_slice_in_dim(rows_padded, first, block_row_list + 2 * border_width, 1)
        row_valid = lax.dynamic_slice_in_dim(rvalid_padded, first, block_row_list + 2 * border_width, 0)
        span = block_row_list + DIAGONAL_COUNT + 4 * border_width - 1
        col_window = lax.dynamic_slice_in_dim(cols_padded, first, span, 1)
        col_valid = lax.dynamic_slice_in_dim(cvalid_padded, first, span, 0)
        hidden_ext, valid_ext, active_extended = pair_block(row_embed, row_valid, col_window, col_valid, -border_width, block_row_list + 2 * border_width, DIAGONAL_COUNT + 2 * border_width, band_limit)
        hidden = hidden_ext[:, border_width:border_width + block_row_list, border_width:border_width + DIAGONAL_COUNT]
        validity = valid_ext[border_width:border_width + block_row_list, border_width:border_width + DIAGONAL_COUNT]
        mixed_features = dilated_convolve(active_extended, kernel, dilation_factor, block_row_list, DIAGONAL_COUNT, border_width) + bias[:, None, None]
        output = ((hidden + mixed_features) * validity).astype(jnp.bfloat16)
        corner_patch = (jnp.int32(0), first, jnp.int32(0))
        grad_window = lax.dynamic_slice(grad_padded, corner_patch, (channels, block_row_list + 2 * border_width, DIAGONAL_COUNT + 2 * border_width))
        gradient_extended = (grad_window.astype(jnp.float32) * valid_ext).astype(jnp.bfloat16)
        gradient_local = gradient_extended[:, border_width:border_width + block_row_list, border_width:border_width + DIAGONAL_COUNT]
        kernel_portion = kernel_summands(gradient_local, active_extended, dilation_factor, block_row_list, DIAGONAL_COUNT, border_width)
        bias_part = lax.optimization_barrier(jnp.sum(gradient_local.astype(jnp.float32), axis=(1, 2)))
        activation_grad = dilated_convolve_grad(gradient_extended, kernel, dilation_factor, block_row_list, DIAGONAL_COUNT, border_width)
        unused, pullback = jax.vjp(jax.nn.gelu, hidden)
        dpair = (gradient_local.astype(jnp.float32) + pullback(activation_grad * validity)[0]) * validity
        row_part = lax.optimization_barrier(jnp.sum(dpair, axis=2))
        col_part = diagonal_sums(dpair)
        current = lax.dynamic_slice_in_dim(col_totals, first, block_row_list + DIAGONAL_COUNT - 1, 1)
        col_totals = lax.dynamic_update_slice_in_dim(col_totals, current + col_part, first, 1)
        return ((col_totals, kernel_total + kernel_portion, bias_total + bias_part), (output, row_part))
    start = (jnp.zeros((channels, LENGTH + DIAGONAL_COUNT + block_row_list), jnp.float32), jnp.zeros((3, 3, channels, channels), jnp.float32), jnp.zeros((channels,), jnp.float32))
    count = LENGTH // block_row_list
    final, stacked = lax.scan(advance, start, jnp.arange(count, dtype=jnp.int32))
    col_totals, kernel_total, bias_total = final
    outputs, row_parts = stacked
    pair_out = jnp.transpose(outputs, (1, 0, 2, 3)).reshape(channels, LENGTH, DIAGONAL_COUNT)
    row_sum = jnp.transpose(row_parts, (1, 0, 2)).reshape(channels, LENGTH)
    embed_scale = 1.0 / jnp.sqrt(jnp.float32(DIAGONAL_COUNT))
    weight_scale = 1.0 / jnp.sqrt(jnp.float32(LENGTH) * jnp.float32(DIAGONAL_COUNT))
    return (pair_out, row_sum * embed_scale, col_totals[:, :LENGTH] * embed_scale, kernel_total * weight_scale, bias_total * weight_scale)
```

```python
import functools

import jax
import jax.numpy as jnp
from jax import lax
from jax.experimental import pallas as pl
from jax.experimental.pallas import tpu as pltpu
from jax.sharding import PartitionSpec as P

MAXDIL = 4
RG = 8
S2PI = 0.7978845608028654
CUBIC = 0.044715
bf, f32 = jnp.bfloat16, jnp.float32


def loop(count, body):
    def step(p, c):
        body(p)
        return c
    lax.fori_loop(0, count, step, 0)


def send(src, dst, ss, sr, dq, dt):
    return pltpu.make_async_remote_copy(
        src_ref=src, dst_ref=dst, send_sem=ss, recv_sem=sr,
        device_id={"row": dq, "diag": dt}, device_id_type=pl.DeviceIdType.MESH,
    )


def gelu_parts(h):
    h2 = h * h
    t = jnp.tanh(h * (S2PI + (S2PI * CUBIC) * h2))
    cdf = 0.5 + 0.5 * t
    return h2, t, cdf


def divisor(total, limit):
    return max(k for k in range(1, limit + 1) if total % k == 0)


def fused_kernel(
    R, T, embed_scale, weight_scale,
    dilation, band, rows, cols, valid, kf, bias, cot,
    out, kres, rcres,
    pack, blocks, cf, ct, edge_l, edge_r, from_r, from_l,
    cw, nr, hlc, hlr, hact, hval,
    act5, gz5, gzm, hid, der, vb, vb16, yz, yd, wz, wd, kacc, bacc, kg, row, col,
    kbuf, rbuf, abuf, bbuf, ksum, rcsum,
    ps, pr, hs, hr, ks, kr, rs, rr, as_, ar, bs, br, k2s, k2r, r2s, r2r,
):
    ch, n = rows.shape
    m = MAXDIL
    width = 2 * m
    per = n // width
    tiles = n // per
    ext = n + 2 * m
    stride = cf.shape[0] // ch
    N = R * T
    K, Z = kg.shape[0], row.shape[0]
    q, t = lax.axis_index("row"), lax.axis_index("diag")
    me = q * T + t
    r, w = dilation[0], band[0]
    mesh_id = pl.DeviceIdType.MESH
    barrier = pltpu.get_barrier_semaphore()
    left, right, above, below = t > 0, t < T - 1, q > 0, q < R - 1

    def greet(p):
        @pl.when(p != me)
        def _():
            pl.semaphore_signal(barrier, inc=1, device_id={"row": p // T, "diag": p % T}, device_id_type=mesh_id)
    loop(N, greet)

    pack[0:ch] = cols[...]
    pack[ch : 2 * ch] = rows[...]
    pack[2 * ch : 2 * ch + 16] = jnp.broadcast_to(valid[...].astype(f32), (16, n)).astype(bf)
    zero = jnp.zeros(pack.shape, bf)
    blocks[0] = zero
    for k in range(R + 1, R + T + 3):
        blocks[k] = zero
    blocks[q + 1] = pack[...]
    pl.semaphore_wait(barrier, N - 1)

    def p1(p):
        return send(pack, blocks.at[q + 1], ps.at[p], pr.at[q], p, t)

    def peers(act):
        def one(p):
            @pl.when(p != q)
            def _():
                act(p)
        loop(R, one)
    peers(lambda p: p1(p).start())

    lane = lax.broadcasted_iota(jnp.int32, (ch, n), 1)

    def spread(c):
        cf[pl.ds(pl.multiple_of(c * stride, 8), n), :] = cot[c].astype(f32)
    loop(ch, spread)

    def pack_edges(g):
        a = jnp.zeros((ch, n), bf)
        b = jnp.zeros((ch, n), bf)
        for s in range(per):
            i = g * per + s
            x = cf[pl.ds(i, ch, stride=stride), :].astype(bf)
            ct[m + i] = x
            here = lane // width == s
            a = jnp.where(here, pltpu.roll(x, width * s, 1) if s else x, a)
            sh = (width * (s + 1)) % n
            b = jnp.where(here, pltpu.roll(x, sh, 1) if sh else x, b)
        edge_l[g] = a
        edge_r[g] = b
    loop(tiles, pack_edges)

    def halos(act):
        last = tiles - 1
        plan = (
            (left, edge_l, from_r.at[pl.ds(1, tiles)], 0, 0, -1),
            (right, edge_r, from_l.at[pl.ds(1, tiles)], 1, 0, 1),
            (above, ct.at[pl.ds(m, m)], ct.at[pl.ds(n + m, m)], 2, -1, 0),
            (below, ct.at[pl.ds(n, m)], ct.at[pl.ds(0, m)], 3, 1, 0),
            (below & left, edge_l.at[last], from_r.at[0], 4, 1, -1),
            (above & left, edge_l.at[0], from_r.at[tiles + 1], 5, -1, -1),
            (below & right, edge_r.at[last], from_l.at[0], 6, 1, 1),
            (above & right, edge_r.at[0], from_l.at[tiles + 1], 7, -1, 1),
        )
        flags = {(0, -1): right, (0, 1): left, (-1, 0): below, (1, 0): above,
                 (1, -1): above & right, (-1, -1): below & right, (1, 1): above & left, (-1, 1): below & left}
        for ok, src, dst, k, dq, dt in plan:
            act(ok, flags[(dq, dt)], src, dst, send(src, dst, hs.at[k], hr.at[k], q + dq, t + dt))

    def start(ok, got, src, dst, c):
        @pl.when(ok)
        def _():
            c.start()
    halos(start)

    for a in range(3):
        zrow, drow = [None] * 5, [None] * 5
        for b in range(3):
            x = kf[3 * a + b].astype(f32)
            zrow[b - a + 2] = x
            drow[a - b + 2] = x.T
        blank = jnp.zeros((ch, ch), f32)
        fill = lambda xs: jnp.concatenate([blank if x is None else x for x in xs], axis=1).astype(bf)
        wz[a * ch : (a + 1) * ch, :] = fill(zrow)
        wd[a * ch : (a + 1) * ch, :] = fill(drow)

    peers(lambda p: send(pack, blocks.at[p + 1], ps.at[p], pr.at[p], q, t).wait_recv())

    d0 = t * n
    v0 = 2 * ch
    for k in range(4):
        x = blocks[q + t + k].astype(f32)
        cw[k, 0:ch] = x[0:ch]
        cw[k, ch : ch + RG] = x[v0 : v0 + RG]
    for k in range(3):
        x = blocks[q + k].astype(f32)
        nr[k, 0:ch] = x[ch : 2 * ch]
        nr[k, ch : ch + RG] = x[v0 : v0 + RG]

    hrows = ch + 16
    slots = tiles + 2
    lane_h = lax.broadcasted_iota(jnp.int32, (hrows, n), 1)
    cblk = [jnp.concatenate([blocks[q + t + k, 0:ch], blocks[q + t + k, v0 : v0 + 16]], axis=0) for k in range(4)]
    rblk = [jnp.concatenate([blocks[q + k, ch : 2 * ch], blocks[q + k, v0 : v0 + 16]], axis=0) for k in range(3)]

    def window(blks, base):
        k, sh = base // n, base % n
        x = blks[k]
        if sh:
            if k + 1 < len(blks):
                x = jnp.where(lane_h >= sh, x, blks[k + 1])
            x = pltpu.roll(x, n - sh, 1)
        return x
    for g in range(slots):
        for side, off in ((0, 2 * n - per), (1, n - per - width)):
            hlc[(2 * g + side) * hrows : (2 * g + side + 1) * hrows, :] = window(cblk, per * g + off)
        hlr[g * hrows : (g + 1) * hrows, :] = window(rblk, per * g + n - per)
    src = lax.broadcasted_iota(jnp.int32, (n, n), 0)
    dst = lax.broadcasted_iota(jnp.int32, (n, n), 1)
    one = lambda cond: jnp.where(cond, 1.0, 0.0).astype(bf)
    hc = jnp.dot(hlc[...], one(src == dst // width + dst % width), preferred_element_type=f32)
    hw = jnp.dot(hlr[...], one(src == dst // width), preferred_element_type=f32)
    kk = lax.broadcasted_iota(jnp.int32, (RG, n), 1) % width
    for g in range(slots):
        hrw = hw[g * hrows : (g + 1) * hrows]
        for side in range(2):
            hcc = hc[(2 * g + side) * hrows : (2 * g + side + 1) * hrows]
            da = d0 + kk + (-width if side else n)
            v8 = jnp.where((da >= 0) & (da < w), hcc[ch : ch + RG] * hrw[ch : ch + RG], 0.0)
            v = jnp.concatenate([v8] * (ch // RG), axis=0)
            h = (hrw[0:ch] + hcc[0:ch]) * v
            _, _, cdf = gelu_parts(h)
            hact[side, g] = (h * cdf).astype(bf)
            hval[side, g] = jnp.concatenate([v8, v8], axis=0).astype(bf)

    lane8 = lax.broadcasted_iota(jnp.int32, (RG, n), 1)
    lane40 = lax.broadcasted_iota(jnp.int32, (ch + RG, n), 1)

    def shifts(dst, e, main, hright, hleft):
        s = lax.rem(e + per - m, per)
        a = pltpu.roll(hright, lax.rem(n - width * s, n), 1)
        b = pltpu.roll(hleft, lax.rem(2 * n - width - width * s, n), 1)
        hx = jnp.where(lane < n // 2, a, b)
        dst[e, 2 * ch : 3 * ch] = main
        for k in (1, 2):
            sr = k * r
            dst[e, (2 + k) * ch : (3 + k) * ch] = pltpu.roll(jnp.where(lane < sr, hx, main), n - sr, 1)
            dst[e, (2 - k) * ch : (3 - k) * ch] = pltpu.roll(jnp.where(lane >= n - sr, hx, main), sr, 1)

    def phase_a1(gi):
        for ii in range(RG):
            e = gi * RG + ii
            at = e - m + n
            k, sh = at // n, lax.rem(at, n)
            c = pltpu.roll(jnp.where(lane40 >= sh, cw[k], cw[k + 1]), lax.rem(n - sh, n), 1)
            rw = jnp.take_along_axis(nr[k], jnp.full((ch + RG, n), sh, jnp.int32), axis=1)
            v8 = jnp.where(lane8 + d0 < w, c[ch:] * rw[ch:], 0.0)
            vb[e] = v8
            vb16[e] = jnp.concatenate([v8, v8], axis=0).astype(bf)
            v = jnp.concatenate([v8] * (ch // RG), axis=0)
            h = (rw[:ch] + c[:ch]) * v
            h2, tt, cdf = gelu_parts(h)
            hid[e] = h
            der[e] = (cdf + (0.5 * h) * (1.0 - tt * tt) * (S2PI + (3.0 * CUBIC * S2PI) * h2)) * v
            slot = (e + per - m) // per
            shifts(act5, e, (h * cdf).astype(bf), hact[0, slot], hact[1, slot])
    loop(ext // RG, phase_a1)

    def finish(ok, got, src, dst, c):
        @pl.when(got)
        def _():
            c.wait_recv()

        @pl.when(jnp.logical_not(got))
        def _():
            dst[...] = jnp.zeros(dst.shape, bf)
    halos(finish)

    def halo_gz(g):
        for side, buf in ((0, from_r), (1, from_l)):
            x = hval[side, g]
            buf[g] = buf[g] * jnp.concatenate([x, x], axis=0)
    loop(slots, halo_gz)
    bacc[...] = jnp.zeros_like(bacc)
    for e in range(2 * m):
        gzm[e] = jnp.zeros((ch, n), bf)
        gzm[n + 2 * m + e] = jnp.zeros((ch, n), bf)

    def gz_row(e, inner):
        x = vb16[e]
        g = ct[e] * jnp.concatenate([x, x], axis=0)
        slot = (e + per - m) // per
        shifts(gz5, e, g, from_r[slot], from_l[slot])
        if inner:
            gzm[e + m] = g
            return g.astype(f32)

    def phase_a2(gi):
        tot = bacc[...]
        for ii in range(RG):
            tot = tot + gz_row(m + gi * RG + ii, True)
        bacc[...] = tot
    loop(n // RG, phase_a2)

    def outer_rows(s):
        gz_row(s, False)
        gz_row(n + m + s, False)
    loop(m, outer_rows)

    gr = divisor(ext, 34)
    kacc[...] = jnp.zeros_like(kacc)

    def phase_k(gi):
        xs, gs, ys = [], [], []
        for ii in range(gr):
            e = gi * gr + ii
            xs.append(act5[e])
            ys.append(gz5[e])
            gs.append(jnp.concatenate([gzm[e + m - (a - 1) * r] for a in range(3)], axis=0))
        kacc[...] += lax.dot_general(jnp.concatenate(gs, axis=1), jnp.concatenate(xs, axis=1),
                                     (((1,), (1,)), ((), ())), preferred_element_type=f32)
        y = jnp.dot(wd[...], jnp.concatenate(ys, axis=1), preferred_element_type=f32)
        for ii in range(gr):
            yd[gi * gr + ii] = y[:, ii * n : (ii + 1) * n]
    loop(ext // gr, phase_k)

    for a in range(3):
        for b in range(3):
            k = b - a + 2
            x = kacc[a * ch : (a + 1) * ch, k * ch : (k + 1) * ch]
            kg[3 * a + b] = jnp.concatenate([x[z * RG : (z + 1) * RG] for z in range(ch // RG)], axis=1)
    diag = lax.broadcasted_iota(jnp.int32, (ch, n), 0) == lane
    bt = jnp.sum(bacc[...], axis=1, keepdims=True)
    kg[9] = jnp.broadcast_to(jnp.sum(jnp.where(diag, bt, 0.0), axis=0, keepdims=True), (RG, n))

    def phase_b(gi, carry):
        lo, hi, rsum = carry
        for ii in range(RG):
            i = gi * RG + ii
            da = yd[m + i + r, 0:ch] + yd[m + i, ch : 2 * ch] + yd[m + i - r, 2 * ch : 3 * ch]
            dx = gzm[i + 2 * m].astype(f32) + der[m + i] * da
            x = pltpu.roll(dx, i, 1)
            wrap = lane < i
            lo = lo + jnp.where(wrap, 0.0, x)
            hi = hi + jnp.where(wrap, x, 0.0)
            rsum = jnp.where(lane == i, jnp.sum(dx, axis=1, keepdims=True), rsum)
        return lo, hi, rsum
    zf = jnp.zeros((ch, n), f32)
    lo, hi, rsum = lax.fori_loop(0, n // RG, phase_b, (zf, zf, zf))
    for z in range(Z):
        sl = slice(z * RG, (z + 1) * RG)
        row[z] = rsum[sl]
        col[0, z] = lo[sl]
        col[1, z] = hi[sl]

    def k1(k):
        return send(kg.at[k], kbuf.at[me], ks.at[k], kr.at[me], k // T, k % T)

    def r1(z):
        return send(row.at[z], rbuf.at[t], rs.at[z], rr.at[t], q, z)

    def a1(z):
        return send(col.at[0, z], abuf.at[q], as_.at[z], ar.at[q], q + t, z)

    def b1(z):
        return send(col.at[1, z], bbuf.at[q], bs.at[z], br.at[q], q + t + 1, z)

    def first(act):
        for k in range(K):
            @pl.when(me != k)
            def _():
                act(k1(k))
        for z in range(Z):
            @pl.when(t != z)
            def _():
                act(r1(z))

            @pl.when((q + t < R) & ((t != 0) | (z != 0)))
            def _():
                act(a1(z))

            @pl.when(q + t + 1 < R)
            def _():
                act(b1(z))

    first(lambda c: c.start())

    def phase_z(gi):
        x = jnp.concatenate([act5[gi * gr + ii] for ii in range(gr)], axis=1)
        y = jnp.dot(wz[...], x, preferred_element_type=f32)
        for ii in range(gr):
            yz[gi * gr + ii] = y[:, ii * n : (ii + 1) * n]
    loop(ext // gr, phase_z)
    eye = lax.broadcasted_iota(jnp.int32, (ch, ch), 0) == lax.broadcasted_iota(jnp.int32, (ch, ch), 1)
    bcol = jnp.sum(jnp.where(eye, bias[...], 0.0), axis=1, keepdims=True)
    bias_all = jnp.broadcast_to(bcol, (ch, n))

    def phase_o(gi):
        for ii in range(RG):
            i = gi * RG + ii
            z = yz[m + i - r, 0:ch] + yz[m + i, ch : 2 * ch] + yz[m + i + r, 2 * ch : 3 * ch]
            v = jnp.concatenate([vb[m + i]] * (ch // RG), axis=0)
            cf[pl.ds(i, ch, stride=stride), :] = (hid[m + i] + z + bias_all) * v
    loop(n // RG, phase_o)

    def emit(c):
        out[c] = cf[pl.ds(pl.multiple_of(c * stride, 8), n), :].astype(bf)
    loop(ch, emit)

    def got(buf, sem):
        send(buf, buf, sem, sem, q, t).wait_recv()

    def k2(p):
        return send(ksum, kres.at[me], k2s.at[p], k2r.at[me], p // T, p % T)

    def r2(p):
        return send(rcsum, rcres.at[t], r2s.at[p], r2r.at[t], q, p)

    def second(act):
        @pl.when(me < K)
        def _():
            def one(p):
                @pl.when(p != me)
                def _():
                    act(k2(p))
            loop(N, one)

        @pl.when(t < Z)
        def _():
            def one(p):
                @pl.when(p != t)
                def _():
                    act(r2(p))
            loop(T, one)

    @pl.when(me < K)
    def _():
        ksum[...] = kg[me]

        def take(p):
            @pl.when(p != me)
            def _():
                got(kbuf.at[p], kr.at[p])
                ksum[...] += kbuf[p]
        loop(N, take)
        ksum[...] = ksum[...] * weight_scale
        kres[me] = ksum[...]

    @pl.when(t < Z)
    def _():
        rcsum[0] = row[t]
        rcsum[1] = jnp.zeros_like(rcsum[1])

        def take(p):
            @pl.when(p != t)
            def _():
                got(rbuf.at[p], rr.at[p])
                rcsum[0] += rbuf[p]
        loop(T, take)

        @pl.when(t == 0)
        def _():
            rcsum[1] = col[0, 0]

        def take_col(p):
            @pl.when((p <= q) & (q - p < T) & ((p != q) | (t != 0)))
            def _():
                got(abuf.at[p], ar.at[p])
                rcsum[1] += abuf[p]

            @pl.when((p <= q - 1) & (q - 1 - p < T))
            def _():
                got(bbuf.at[p], br.at[p])
                rcsum[1] += bbuf[p]
        loop(R, take_col)
        rcsum[...] = rcsum[...] * embed_scale
        rcres[t] = rcsum[...]

    second(lambda c: c.start())
    for k in range(K):
        @pl.when(me != k)
        def _():
            got(kres.at[k], k2r.at[k])
    for z in range(Z):
        @pl.when(t != z)
        def _():
            got(rcres.at[z], r2r.at[z])
    peers(lambda p: p1(p).wait_send())

    def sent(ok, got, src, dst, c):
        @pl.when(ok)
        def _():
            c.wait_send()
    halos(sent)
    first(lambda c: c.wait_send())
    second(lambda c: c.wait_send())


def finish_kernel(pair, kres, rcres, out, row_out, col_out, kg_out, bg_out):
    out[...] = pair[...]
    ch = row_out.shape[0]
    for z in range(ch // RG):
        row_out[z * RG : (z + 1) * RG, :] = rcres[z, 0]
        col_out[z * RG : (z + 1) * RG, :] = rcres[z, 1]
        for s in range(9):
            kg_out[s, z * RG : (z + 1) * RG, :] = kres[s, :, z * ch : (z + 1) * ch]
    bg_out[...] = kres[9, 0:1, 0:ch]


def local(emb_rows, emb_cols, kernel, bias, cotangent, valid, dilation, band):
    ch, n = emb_rows.shape
    R, T = lax.axis_size("row"), lax.axis_size("diag")
    m = MAXDIL
    ext = n + 2 * m
    vmem = pl.BlockSpec(memory_space=pltpu.VMEM)
    smem = pl.BlockSpec(memory_space=pltpu.SMEM)
    dma = pltpu.SemaphoreType.DMA
    V = pltpu.VMEM
    width = 2 * m
    per = n // width
    tiles = n // per
    slots = tiles + 2
    hrows = ch + 16
    kf = kernel.reshape(9, ch, ch)
    nk = (9 * ch * ch) // (RG * 128) + 1
    Z = ch // RG
    tile = lambda *lead: V(lead + (RG, n), f32)
    edges = lambda k: V((k, ch, n), bf)
    embed_scale = float(T * n) ** -0.5
    weight_scale = float(R * n * T * n) ** -0.5
    pair, kres, rcres = pl.pallas_call(
        functools.partial(fused_kernel, R, T, embed_scale, weight_scale),
        out_shape=(
            jax.ShapeDtypeStruct((ch, n, n), bf),
            jax.ShapeDtypeStruct((nk, RG, n), f32),
            jax.ShapeDtypeStruct((Z, 2, RG, n), f32),
        ),
        in_specs=[smem, smem] + [vmem] * 6,
        out_specs=(vmem,) * 3,
        scratch_shapes=[
            V((2 * ch + 16, n), bf), V((R + T + 3, 2 * ch + 16, n), bf), V((ch * (n + 8), n), f32),
            edges(ext), edges(tiles), edges(tiles), edges(slots), edges(slots),
            V((4, ch + RG, n), f32), V((3, ch + RG, n), f32),
            V((slots * 2 * hrows, n), bf), V((slots * hrows, n), bf),
            V((2, slots, ch, n), bf), V((2, slots, 16, n), bf),
            V((ext, 5 * ch, n), bf), V((ext, 5 * ch, n), bf), V((ext + 2 * m, ch, n), bf),
            V((ext, ch, n), f32), V((ext, ch, n), f32), V((ext, RG, n), f32), V((ext, 16, n), bf),
            V((ext, 3 * ch, n), f32), V((ext, 3 * ch, n), f32),
            V((3 * ch, 5 * ch), bf), V((3 * ch, 5 * ch), bf), V((3 * ch, 5 * ch), f32),
            V((ch, n), f32), tile(nk), tile(Z), tile(2, Z),
            tile(R * T), tile(T), tile(R), tile(R), tile(), tile(2),
            dma((R,)), dma((R,)), dma((8,)), dma((8,)),
            dma((nk,)), dma((R * T,)), dma((Z,)), dma((T,)), dma((Z,)), dma((R,)), dma((Z,)), dma((R,)),
            dma((R * T,)), dma((nk,)), dma((T,)), dma((Z,)),
        ],
        compiler_params=pltpu.CompilerParams(collective_id=0, has_side_effects=True, vmem_limit_bytes=56 * 2**20),
        name="fused_kernel",
    )(dilation, band, emb_rows, emb_cols, valid[None, :], kf, bias[None, :], cotangent)

    out, row_grad, col_grad, kgt, bgt = pl.pallas_call(
        finish_kernel,
        out_shape=(
            jax.ShapeDtypeStruct((ch, n, n), bf),
            jax.ShapeDtypeStruct((ch, n), f32),
            jax.ShapeDtypeStruct((ch, n), f32),
            jax.ShapeDtypeStruct((9, ch, ch), f32),
            jax.ShapeDtypeStruct((1, ch), f32),
        ),
        in_specs=[vmem] * 3,
        out_specs=(vmem,) * 5,
        name="finish_kernel",
    )(pair, kres, rcres)
    return out, row_grad, col_grad, kgt.reshape(3, 3, ch, ch), bgt.reshape(ch)


def solution(mesh):
    in_specs = (
        P(None, ("grp", "row")),
        P(None, ("grp", "row")),
        P(),
        P(),
        P(None, ("grp", "row"), "diag"),
        P(("grp", "row")),
        P("grp"),
        P("grp"),
    )
    out_specs = (
        P(None, ("grp", "row"), "diag"),
        P(None, ("grp", "row")),
        P(None, ("grp", "row")),
        P("grp", None, None, None),
        P("grp"),
    )
    return jax.shard_map(local, mesh=mesh, in_specs=in_specs, out_specs=out_specs, check_vma=False)
```

```python
import functools

import jax
import jax.numpy as jnp
from jax import lax
from jax.experimental import pallas as pl
from jax.experimental.pallas import tpu as pltpu
from jax.sharding import PartitionSpec as P

MAXDIL = 4
RG = 8
S2PI = 0.7978845608028654
CUBIC = 0.044715
bf, f32 = jnp.bfloat16, jnp.float32


def loop(count, body):
    def step(p, c):
        body(p)
        return c
    lax.fori_loop(0, count, step, 0)


def send(src, dst, ss, sr, dq, dt):
    return pltpu.make_async_remote_copy(
        src_ref=src, dst_ref=dst, send_sem=ss, recv_sem=sr,
        device_id={"row": dq, "diag": dt}, device_id_type=pl.DeviceIdType.MESH,
    )


def gelu_parts(h):
    h2 = h * h
    t = jnp.tanh(h * (S2PI + (S2PI * CUBIC) * h2))
    cdf = 0.5 + 0.5 * t
    return h2, t, cdf


def divisor(total, limit):
    return max(k for k in range(1, limit + 1) if total % k == 0)


def fused_kernel(
    R, T, embed_scale, weight_scale,
    dilation, band, rows, cols, valid, kf, bias, cot,
    out, kres, rcres,
    pack, blocks, cf, ct, edge_l, edge_r, from_r, from_l, top, bottom,
    cw, rb, hlc, hlr, hpk, hval, um, ha, hg,
    act5, gz5, gzm, hid, der, vb, vb16, yz, yd, wz, wd, kacc, csum, kg, row, col,
    kbuf, rbuf, abuf, bbuf, ksum, rcsum,
    ps, pr, hs, hr, ks, kr, rs, rr, as_, ar, bs, br, k2s, k2r, r2s, r2r,
):
    ch, n = rows.shape
    m = MAXDIL
    width = 2 * m
    per = n // width
    tiles = n // per
    ext = n + 2 * m
    stride = cf.shape[0] // ch
    N = R * T
    K, Z = kg.shape[0], row.shape[0]
    q, t = lax.axis_index("row"), lax.axis_index("diag")
    me = q * T + t
    r, w = dilation[0], band[0]
    mesh_id = pl.DeviceIdType.MESH
    barrier = pltpu.get_barrier_semaphore()
    left, right, above, below = t > 0, t < T - 1, q > 0, q < R - 1

    def greet(p):
        @pl.when(p != me)
        def _():
            pl.semaphore_signal(barrier, inc=1, device_id={"row": p // T, "diag": p % T}, device_id_type=mesh_id)
    loop(N, greet)

    pack[0:ch] = cols[...]
    pack[ch : 2 * ch] = rows[...]
    pack[2 * ch : 2 * ch + 16] = jnp.broadcast_to(valid[...].astype(f32), (16, n)).astype(bf)
    zero = jnp.zeros(pack.shape, bf)
    blocks[0] = zero
    for k in range(R + 1, R + T + 3):
        blocks[k] = zero
    blocks[q + 1] = pack[...]
    pl.semaphore_wait(barrier, N - 1)

    def p1(p):
        return send(pack, blocks.at[q + 1], ps.at[p], pr.at[q], p, t)

    def peers(act):
        def one(p):
            @pl.when(p != q)
            def _():
                act(p)
        loop(R, one)
    peers(lambda p: p1(p).start())

    lane = lax.broadcasted_iota(jnp.int32, (ch, n), 1)

    def spread(c):
        cf[pl.ds(pl.multiple_of(c * stride, 8), n), :] = cot[c].astype(f32)
    loop(ch, spread)

    def pack_edges(g):
        a = jnp.zeros((ch, n), bf)
        b = jnp.zeros((ch, n), bf)
        for s in range(per):
            i = g * per + s
            x = cf[pl.ds(i, ch, stride=stride), :].astype(bf)
            ct[m + i] = x
            here = lane // width == s
            a = jnp.where(here, pltpu.roll(x, width * s, 1) if s else x, a)
            sh = (width * (s + 1)) % n
            b = jnp.where(here, pltpu.roll(x, sh, 1) if sh else x, b)
        edge_l[g] = a
        edge_r[g] = b
    loop(tiles, pack_edges)

    def halos(act):
        last = tiles - 1
        plan = (
            (left, edge_l, from_r.at[pl.ds(1, tiles)], 0, 0, -1),
            (right, edge_r, from_l.at[pl.ds(1, tiles)], 1, 0, 1),
            (above, ct.at[pl.ds(m, m)], bottom, 2, -1, 0),
            (below, ct.at[pl.ds(n, m)], top, 3, 1, 0),
            (below & left, edge_l.at[last], from_r.at[0], 4, 1, -1),
            (above & left, edge_l.at[0], from_r.at[tiles + 1], 5, -1, -1),
            (below & right, edge_r.at[last], from_l.at[0], 6, 1, 1),
            (above & right, edge_r.at[0], from_l.at[tiles + 1], 7, -1, 1),
        )
        flags = {(0, -1): right, (0, 1): left, (-1, 0): below, (1, 0): above,
                 (1, -1): above & right, (-1, -1): below & right, (1, 1): above & left, (-1, 1): below & left}
        for ok, src, dst, k, dq, dt in plan:
            act(ok, flags[(dq, dt)], src, dst, send(src, dst, hs.at[k], hr.at[k], q + dq, t + dt))

    def start(ok, got, src, dst, c):
        @pl.when(ok)
        def _():
            c.start()
    halos(start)

    for s in range(per):
        p = lax.broadcasted_iota(jnp.int32, (2 * n, n), 0)
        x = lax.broadcasted_iota(jnp.int32, (2 * n, n), 1)
        pick = ((p == width * s + x) & (x < width)) | ((p == width * s + x + width) & (x >= n - width) & (p >= n))
        um[:, s * n : (s + 1) * n] = jnp.where(pick, 1.0, 0.0).astype(bf)

    for a in range(3):
        zrow, drow = [None] * 5, [None] * 5
        for b in range(3):
            x = kf[3 * a + b].astype(f32)
            zrow[b - a + 2] = x
            drow[a - b + 2] = x.T
        blank = jnp.zeros((ch, ch), f32)
        fill = lambda xs: jnp.concatenate([blank if x is None else x for x in xs], axis=1).astype(bf)
        wz[a * ch : (a + 1) * ch, :] = fill(zrow)
        wd[a * ch : (a + 1) * ch, :] = fill(drow)

    peers(lambda p: send(pack, blocks.at[p + 1], ps.at[p], pr.at[p], q, t).wait_recv())

    d0 = t * n
    v0 = 2 * ch
    for k in range(4):
        x = blocks[q + t + k].astype(f32)
        cw[k, 0:ch] = x[0:ch]
        cw[k, ch : ch + RG] = x[v0 : v0 + RG]
    hrows = ch + 16
    slots = tiles + 2
    lane_h = lax.broadcasted_iota(jnp.int32, (hrows, n), 1)
    cblk = [jnp.concatenate([blocks[q + t + k, 0:ch], blocks[q + t + k, v0 : v0 + 16]], axis=0) for k in range(4)]
    rblk = [jnp.concatenate([blocks[q + k, ch : 2 * ch], blocks[q + k, v0 : v0 + 16]], axis=0) for k in range(3)]

    for k in range(3):
        rb[k] = rblk[k]

    def window(blks, base):
        k, sh = base // n, base % n
        x = blks[k]
        if sh:
            if k + 1 < len(blks):
                x = jnp.where(lane_h >= sh, x, blks[k + 1])
            x = pltpu.roll(x, n - sh, 1)
        return x
    for g in range(slots):
        for side, off in ((0, 2 * n - per), (1, n - per - width)):
            hlc[(2 * g + side) * hrows : (2 * g + side + 1) * hrows, :] = window(cblk, per * g + off)
        hlr[g * hrows : (g + 1) * hrows, :] = window(rblk, per * g + n - per)
    src = lax.broadcasted_iota(jnp.int32, (n, n), 0)
    dst = lax.broadcasted_iota(jnp.int32, (n, n), 1)
    one = lambda cond: jnp.where(cond, 1.0, 0.0).astype(bf)
    hc = jnp.dot(hlc[...], one(src == dst // width + dst % width), preferred_element_type=f32)
    hw = jnp.dot(hlr[...], one(src == dst // width), preferred_element_type=f32)
    kk = lax.broadcasted_iota(jnp.int32, (RG, n), 1) % width
    for g in range(slots):
        hrw = hw[g * hrows : (g + 1) * hrows]
        for side in range(2):
            hcc = hc[(2 * g + side) * hrows : (2 * g + side + 1) * hrows]
            da = d0 + kk + (-width if side else n)
            v8 = jnp.where((da >= 0) & (da < w), hcc[ch : ch + RG] * hrw[ch : ch + RG], 0.0)
            v = jnp.concatenate([v8] * (ch // RG), axis=0)
            h = (hrw[0:ch] + hcc[0:ch]) * v
            _, _, cdf = gelu_parts(h)
            hpk[g * ch : (g + 1) * ch, side * n : (side + 1) * n] = (h * cdf).astype(bf)
            hval[side, g] = jnp.concatenate([v8, v8], axis=0).astype(bf)

    lane8 = lax.broadcasted_iota(jnp.int32, (RG, n), 1)
    lane40 = lax.broadcasted_iota(jnp.int32, (ch + RG, n), 1)
    lane16 = lax.broadcasted_iota(jnp.int32, (16, n), 1)
    sub16 = lax.broadcasted_iota(jnp.int32, (16, n), 0)

    def unpack(dst):
        for j in range(per // 2):
            y = jnp.dot(hpk[...], um[:, 2 * j * n : 2 * (j + 1) * n], preferred_element_type=f32)
            for g in range(slots):
                for s in range(2):
                    dst[g * per + 2 * j + s] = y[g * ch : (g + 1) * ch, s * n : (s + 1) * n].astype(bf)
    unpack(ha)

    def shifts(dst, halo, gi):
        for ii in range(RG):
            e = gi * RG + ii
            hx, main = halo[e + per - m], dst[e, 2 * ch : 3 * ch]
            for k in (1, 2):
                sr = k * r
                dst[e, (2 + k) * ch : (3 + k) * ch] = pltpu.roll(jnp.where(lane < sr, hx, main), n - sr, 1)
                dst[e, (2 - k) * ch : (3 - k) * ch] = pltpu.roll(jnp.where(lane >= n - sr, hx, main), sr, 1)

    ones = jnp.ones((n, n), bf)

    def prep(gi):
        picks, vrow, where_at = [], jnp.zeros((16, n), bf), []
        for ii in range(RG):
            at = gi * RG + ii - m + n
            k, sh = at // n, lax.rem(at, n)
            where_at.append((k, sh))
            x = rb[k]
            picks.append(jnp.where(lane == sh, x[:ch], 0.0))
            vrow = jnp.where((sub16 == ii) & (lane16 == sh), x[ch:], vrow)
        rw = jnp.dot(jnp.concatenate(picks + [vrow], axis=0), ones, preferred_element_type=f32)
        for ii in range(RG):
            e = gi * RG + ii
            k, sh = where_at[ii]
            c = pltpu.roll(jnp.where(lane40 >= sh, cw[k], cw[k + 1]), (n - sh) & (n - 1), 1)
            vr = rw[RG * ch + ii : RG * ch + ii + 1]
            v8 = jnp.where(lane8 + d0 < w, c[ch:] * vr, 0.0)
            vb[e] = v8
            x = jnp.concatenate([v8, v8], axis=0).astype(bf)
            vb16[e] = x
            hid[e] = (rw[ii * ch : (ii + 1) * ch] + c[:ch]) * jnp.concatenate([v8] * (ch // RG), axis=0)
            gzm[e + m] = ct[e] * jnp.concatenate([x, x], axis=0)

    def gelus(gi):
        for ii in range(RG):
            e = gi * RG + ii
            h = hid[e]
            h2 = h * h
            cdf = 0.5 + 0.5 * jnp.tanh(h * (S2PI + (S2PI * CUBIC) * h2))
            act5[e, 2 * ch : 3 * ch] = (h * cdf).astype(bf)
            x = h * (2.0 * S2PI + (6.0 * S2PI * CUBIC) * h2)
            cv = cdf * jnp.concatenate([vb[e]] * (ch // RG), axis=0)
            der[e] = cv + cv * ((1.0 - cdf) * x)

    def kgrad(gi):
        xs, gs = [], []
        for ii in range(RG):
            e = gi * RG + ii
            xs.append(act5[e])
            gs.append(jnp.concatenate([gzm[e + m - (a - 1) * r] for a in range(3)], axis=0))
        kacc[...] += lax.dot_general(jnp.concatenate(gs, axis=1), jnp.concatenate(xs, axis=1),
                                     (((1,), (1,)), ((), ())), preferred_element_type=f32)

    def pipeline(stages, counts, lags):
        first_full = max(lags)
        last_full = min(c + l for c, l in zip(counts, lags))
        total = max(c + l for c, l in zip(counts, lags))

        def at_step(j):
            for f, c, l in zip(stages, counts, lags):
                if 0 <= j - l < c:
                    f(j - l)
        for j in range(first_full):
            at_step(j)

        def body(j):
            for f, l in zip(stages, lags):
                f(j + first_full - l)
        loop(last_full - first_full, body)
        for j in range(last_full, total):
            at_step(j)

    ge, gm = ext // RG, n // RG
    kacc[...] = jnp.zeros_like(kacc)
    for e in range(m):
        gzm[e] = jnp.zeros((ch, n), bf)
        gzm[n + 3 * m + e] = jnp.zeros((ch, n), bf)
    for e in range(m):
        ct[e] = jnp.zeros((ch, n), bf)
        ct[n + m + e] = jnp.zeros((ch, n), bf)
    pipeline((kgrad, lambda g: shifts(act5, ha, g), gelus, prep), (ge,) * 4, (3, 2, 1, 0))

    def bsums(gi, tot):
        for ii in range(2 * RG):
            tot = tot + gzm[2 * m + gi * 2 * RG + ii].astype(f32)
        return tot
    btot = lax.fori_loop(0, n // (2 * RG), bsums, jnp.zeros((ch, n), f32))

    for a in range(3):
        for b in range(3):
            k = b - a + 2
            x = kacc[a * ch : (a + 1) * ch, k * ch : (k + 1) * ch]
            kg[3 * a + b] = jnp.concatenate([x[z * RG : (z + 1) * RG] for z in range(ch // RG)], axis=1)
    diag = lax.broadcasted_iota(jnp.int32, (ch, n), 0) == lane
    bt = jnp.sum(btot, axis=1, keepdims=True)
    kg[9] = jnp.broadcast_to(jnp.sum(jnp.where(diag, bt, 0.0), axis=0, keepdims=True), (RG, n))

    def k1(k):
        return send(kg.at[k], kbuf.at[me], ks.at[k], kr.at[me], k // T, k % T)

    def first_k(act):
        for k in range(K):
            @pl.when(me != k)
            def _():
                act(k1(k))
    first_k(lambda c: c.start())

    def finish(ok, got, src, dst, c):
        @pl.when(got)
        def _():
            c.wait_recv()

        @pl.when(jnp.logical_not(got))
        def _():
            dst[...] = jnp.zeros(dst.shape, bf)
    halos(finish)

    for g in range(slots):
        for side, buf in ((0, from_r), (1, from_l)):
            x = hval[side, g]
            hpk[g * ch : (g + 1) * ch, side * n : (side + 1) * n] = buf[g] * jnp.concatenate([x, x], axis=0)
    unpack(hg)
    for e in range(m):
        for buf, at in ((top, e), (bottom, n + m + e)):
            x = vb16[at]
            gz5[at, 2 * ch : 3 * ch] = buf[e] * jnp.concatenate([x, x], axis=0)

    def gz_main(gi):
        for ii in range(2 * RG):
            e = m + gi * 2 * RG + ii
            gz5[e, 2 * ch : 3 * ch] = gzm[e + m]
    loop(n // (2 * RG), gz_main)

    def conv_d(gi):
        y = jnp.dot(wd[...], jnp.concatenate([gz5[gi * RG + ii] for ii in range(RG)], axis=1), preferred_element_type=f32)
        for ii in range(RG):
            yd[gi * RG + ii] = y[:, ii * n : (ii + 1) * n]

    csum[...] = jnp.zeros_like(csum)

    def backward(gi):
        lo, hi = csum[0], csum[1]
        for ii in range(RG):
            i = gi * RG + ii
            da = yd[m + i + r, 0:ch] + yd[m + i, ch : 2 * ch] + yd[m + i - r, 2 * ch : 3 * ch]
            dx = gzm[i + 2 * m].astype(f32) + der[m + i] * da
            der[m + i] = dx
            x = pltpu.roll(dx, i, 1)
            wrap = lane < i
            lo = lo + jnp.where(wrap, 0.0, x)
            hi = hi + jnp.where(wrap, x, 0.0)
        csum[0] = lo
        csum[1] = hi
    pipeline((backward, conv_d, lambda g: shifts(gz5, hg, g)), (gm, ge, ge), (3, 1, 0))
    lo, hi = csum[0], csum[1]

    def row_sums(gi, rsum):
        for ii in range(2 * RG):
            i = gi * 2 * RG + ii
            rsum = jnp.where(lane == i, jnp.sum(der[m + i], axis=1, keepdims=True), rsum)
        return rsum
    rsum = lax.fori_loop(0, n // (2 * RG), row_sums, jnp.zeros((ch, n), f32))
    for z in range(Z):
        sl = slice(z * RG, (z + 1) * RG)
        row[z] = rsum[sl]
        col[0, z] = lo[sl]
        col[1, z] = hi[sl]

    def r1(z):
        return send(row.at[z], rbuf.at[t], rs.at[z], rr.at[t], q, z)

    def a1(z):
        return send(col.at[0, z], abuf.at[q], as_.at[z], ar.at[q], q + t, z)

    def b1(z):
        return send(col.at[1, z], bbuf.at[q], bs.at[z], br.at[q], q + t + 1, z)

    def first(act):
        for z in range(Z):
            @pl.when(t != z)
            def _():
                act(r1(z))

            @pl.when((q + t < R) & ((t != 0) | (z != 0)))
            def _():
                act(a1(z))

            @pl.when(q + t + 1 < R)
            def _():
                act(b1(z))

    first(lambda c: c.start())

    def got(buf, sem):
        send(buf, buf, sem, sem, q, t).wait_recv()

    def k2(p):
        return send(ksum, kres.at[me], k2s.at[p], k2r.at[me], p // T, p % T)

    def second_k(act):
        @pl.when(me < K)
        def _():
            def one(p):
                @pl.when(p != me)
                def _():
                    act(k2(p))
            loop(N, one)

    @pl.when(me < K)
    def _():
        ksum[...] = kg[me]

        def take(p):
            @pl.when(p != me)
            def _():
                got(kbuf.at[p], kr.at[p])
                ksum[...] += kbuf[p]
        loop(N, take)
        ksum[...] = ksum[...] * weight_scale
        kres[me] = ksum[...]
    second_k(lambda c: c.start())

    def conv_z(gi):
        y = jnp.dot(wz[...], jnp.concatenate([act5[gi * RG + ii] for ii in range(RG)], axis=1), preferred_element_type=f32)
        for ii in range(RG):
            yz[gi * RG + ii] = y[:, ii * n : (ii + 1) * n]

    eye = lax.broadcasted_iota(jnp.int32, (ch, ch), 0) == lax.broadcasted_iota(jnp.int32, (ch, ch), 1)
    bcol = jnp.sum(jnp.where(eye, bias[...], 0.0), axis=1, keepdims=True)
    bias_all = jnp.broadcast_to(bcol, (ch, n))

    def phase_o(gi):
        for ii in range(RG):
            i = gi * RG + ii
            z = yz[m + i - r, 0:ch] + yz[m + i, ch : 2 * ch] + yz[m + i + r, 2 * ch : 3 * ch]
            v = jnp.concatenate([vb[m + i]] * (ch // RG), axis=0)
            cf[pl.ds(i, ch, stride=stride), :] = (hid[m + i] + z + bias_all) * v
    pipeline((phase_o, conv_z), (gm, ge), (2, 0))

    def emit(c):
        out[c] = cf[pl.ds(pl.multiple_of(c * stride, 8), n), :].astype(bf)
    loop(ch, emit)

    def r2(p):
        return send(rcsum, rcres.at[t], r2s.at[p], r2r.at[t], q, p)

    def second(act):
        @pl.when(t < Z)
        def _():
            def one(p):
                @pl.when(p != t)
                def _():
                    act(r2(p))
            loop(T, one)

    @pl.when(t < Z)
    def _():
        rcsum[0] = row[t]
        rcsum[1] = jnp.zeros_like(rcsum[1])

        def take(p):
            @pl.when(p != t)
            def _():
                got(rbuf.at[p], rr.at[p])
                rcsum[0] += rbuf[p]
        loop(T, take)

        @pl.when(t == 0)
        def _():
            rcsum[1] = col[0, 0]

        def take_col(p):
            @pl.when((p <= q) & (q - p < T) & ((p != q) | (t != 0)))
            def _():
                got(abuf.at[p], ar.at[p])
                rcsum[1] += abuf[p]

            @pl.when((p <= q - 1) & (q - 1 - p < T))
            def _():
                got(bbuf.at[p], br.at[p])
                rcsum[1] += bbuf[p]
        loop(R, take_col)
        rcsum[...] = rcsum[...] * embed_scale
        rcres[t] = rcsum[...]

    second(lambda c: c.start())
    for k in range(K):
        @pl.when(me != k)
        def _():
            got(kres.at[k], k2r.at[k])
    for z in range(Z):
        @pl.when(t != z)
        def _():
            got(rcres.at[z], r2r.at[z])
    peers(lambda p: p1(p).wait_send())

    def sent(ok, got, src, dst, c):
        @pl.when(ok)
        def _():
            c.wait_send()
    halos(sent)
    first_k(lambda c: c.wait_send())
    first(lambda c: c.wait_send())
    second_k(lambda c: c.wait_send())
    second(lambda c: c.wait_send())


def finish_kernel(pair, kres, rcres, out, row_out, col_out, kg_out, bg_out, sem):
    copy = pltpu.make_async_copy(pair, out, sem)
    copy.start()
    ch = row_out.shape[0]
    for z in range(ch // RG):
        row_out[z * RG : (z + 1) * RG, :] = rcres[z, 0]
        col_out[z * RG : (z + 1) * RG, :] = rcres[z, 1]
        for s in range(9):
            kg_out[s, z * RG : (z + 1) * RG, :] = kres[s, :, z * ch : (z + 1) * ch]
    bg_out[...] = kres[9, 0:1, 0:ch]
    copy.wait()


def local(emb_rows, emb_cols, kernel, bias, cotangent, valid, dilation, band):
    ch, n = emb_rows.shape
    R, T = lax.axis_size("row"), lax.axis_size("diag")
    m = MAXDIL
    ext = n + 2 * m
    vmem = pl.BlockSpec(memory_space=pltpu.VMEM)
    smem = pl.BlockSpec(memory_space=pltpu.SMEM)
    dma = pltpu.SemaphoreType.DMA
    V = pltpu.VMEM
    width = 2 * m
    per = n // width
    tiles = n // per
    slots = tiles + 2
    hrows = ch + 16
    kf = kernel.reshape(9, ch, ch)
    nk = (9 * ch * ch) // (RG * 128) + 1
    Z = ch // RG
    tile = lambda *lead: V(lead + (RG, n), f32)
    edges = lambda k: V((k, ch, n), bf)
    embed_scale = float(T * n) ** -0.5
    weight_scale = float(R * n * T * n) ** -0.5
    pair, kres, rcres = pl.pallas_call(
        functools.partial(fused_kernel, R, T, embed_scale, weight_scale),
        out_shape=(
            V((ch, n, n), bf),
            V((nk, RG, n), f32),
            V((Z, 2, RG, n), f32),
        ),
        in_specs=[smem, smem] + [vmem] * 6,
        out_specs=(vmem,) * 3,
        scratch_shapes=[
            V((2 * ch + 16, n), bf), V((R + T + 3, 2 * ch + 16, n), bf), V((ch * (n + 8), n), f32),
            edges(ext), edges(tiles), edges(tiles), edges(slots), edges(slots), edges(m), edges(m),
            V((4, ch + RG, n), f32), V((3, ch + 16, n), bf),
            V((slots * 2 * hrows, n), bf), V((slots * hrows, n), bf),
            V((slots * ch, 2 * n), bf), V((2, slots, 16, n), bf), V((2 * n, per * n), bf), edges(slots * per), edges(slots * per),
            V((ext, 5 * ch, n), bf), V((ext, 5 * ch, n), bf), V((ext + 2 * m, ch, n), bf),
            V((ext, ch, n), f32), V((ext, ch, n), f32), V((ext, RG, n), f32), V((ext, 16, n), bf),
            V((ext, 3 * ch, n), f32), V((ext, 3 * ch, n), f32),
            V((3 * ch, 5 * ch), bf), V((3 * ch, 5 * ch), bf), V((3 * ch, 5 * ch), f32),
            V((2, ch, n), f32), tile(nk), tile(Z), tile(2, Z),
            tile(R * T), tile(T), tile(R), tile(R), tile(), tile(2),
            dma((R,)), dma((R,)), dma((8,)), dma((8,)),
            dma((nk,)), dma((R * T,)), dma((Z,)), dma((T,)), dma((Z,)), dma((R,)), dma((Z,)), dma((R,)),
            dma((R * T,)), dma((nk,)), dma((T,)), dma((Z,)),
        ],
        compiler_params=pltpu.CompilerParams(collective_id=0, has_side_effects=True, vmem_limit_bytes=56 * 2**20),
        name="fused_kernel",
    )(dilation, band, emb_rows, emb_cols, valid[None, :], kf, bias[None, :], cotangent)

    out, row_grad, col_grad, kgt, bgt = pl.pallas_call(
        finish_kernel,
        out_shape=(
            jax.ShapeDtypeStruct((ch, n, n), bf),
            jax.ShapeDtypeStruct((ch, n), f32),
            jax.ShapeDtypeStruct((ch, n), f32),
            jax.ShapeDtypeStruct((9, ch, ch), f32),
            jax.ShapeDtypeStruct((1, ch), f32),
        ),
        in_specs=[vmem] * 3,
        out_specs=(pl.BlockSpec(memory_space=pl.ANY),) + (vmem,) * 4,
        scratch_shapes=[pltpu.SemaphoreType.DMA],
        name="finish_kernel",
    )(*(pltpu.with_memory_space_constraint(x, V) for x in (pair, kres, rcres)))
    return out, row_grad, col_grad, kgt.reshape(3, 3, ch, ch), bgt.reshape(ch)


def solution(mesh):
    in_specs = (
        P(None, ("grp", "row")),
        P(None, ("grp", "row")),
        P(),
        P(),
        P(None, ("grp", "row"), "diag"),
        P(("grp", "row")),
        P("grp"),
        P("grp"),
    )
    out_specs = (
        P(None, ("grp", "row"), "diag"),
        P(None, ("grp", "row")),
        P(None, ("grp", "row")),
        P("grp", None, None, None),
        P("grp"),
    )
    return jax.shard_map(local, mesh=mesh, in_specs=in_specs, out_specs=out_specs, check_vma=False)
```

```python
import functools

import jax
import jax.numpy as jnp
from jax import lax
from jax.experimental import pallas as pl
from jax.experimental.pallas import tpu as pltpu
from jax.sharding import PartitionSpec as P

MAXDIL = 4
RG = 8
S2PI = 0.7978845608028654
CUBIC = 0.044715
bf, f32 = jnp.bfloat16, jnp.float32


def loop(count, body):
    def step(p, c):
        body(p)
        return c
    lax.fori_loop(0, count, step, 0)


def send(src, dst, ss, sr, dq, dt):
    return pltpu.make_async_remote_copy(
        src_ref=src, dst_ref=dst, send_sem=ss, recv_sem=sr,
        device_id={"row": dq, "diag": dt}, device_id_type=pl.DeviceIdType.MESH,
    )


def gelu_parts(h):
    h2 = h * h
    t = jnp.tanh(h * (S2PI + (S2PI * CUBIC) * h2))
    cdf = 0.5 + 0.5 * t
    return h2, t, cdf


def divisor(total, limit):
    return max(k for k in range(1, limit + 1) if total % k == 0)


def fused_kernel(
    R, T, embed_scale, weight_scale,
    dilation, band, rows, cols, valid, kf, bias, cot,
    out, kres, rcres,
    pack, blocks, cf, ct, edge_l, edge_r, from_r, from_l, top, bottom,
    cw, rb, hlc, hlr, hpk, hval, um, ha, hg,
    act5, gz5, actm, hh, hid, der, vb, vb16, yz, yd, wz, wd, kacc, csum, kg, row, col,
    kbuf, rbuf, abuf, bbuf, ksum, rcsum,
    ps, pr, hs, hr, ks, kr, rs, rr, as_, ar, bs, br, k2s, k2r, r2s, r2r,
):
    ch, n = rows.shape
    m = MAXDIL
    width = 2 * m
    per = n // width
    tiles = n // per
    ext = n + 2 * m
    stride = cf.shape[0] // ch
    N = R * T
    K, Z = kg.shape[0], row.shape[0]
    q, t = lax.axis_index("row"), lax.axis_index("diag")
    me = q * T + t
    r, w = dilation[0], band[0]
    mesh_id = pl.DeviceIdType.MESH
    barrier = pltpu.get_barrier_semaphore()
    left, right, above, below = t > 0, t < T - 1, q > 0, q < R - 1

    def greet(p):
        @pl.when(p != me)
        def _():
            pl.semaphore_signal(barrier, inc=1, device_id={"row": p // T, "diag": p % T}, device_id_type=mesh_id)
    loop(N, greet)

    pack[0:ch] = cols[...]
    pack[ch : 2 * ch] = rows[...]
    pack[2 * ch : 2 * ch + 16] = jnp.broadcast_to(valid[...].astype(f32), (16, n)).astype(bf)
    zero = jnp.zeros(pack.shape, bf)
    blocks[0] = zero
    for k in range(R + 1, R + T + 3):
        blocks[k] = zero
    blocks[q + 1] = pack[...]
    pl.semaphore_wait(barrier, N - 1)

    def p1(p):
        return send(pack, blocks.at[q + 1], ps.at[p], pr.at[q], p, t)

    def peers(act):
        def one(p):
            @pl.when(p != q)
            def _():
                act(p)
        loop(R, one)
    peers(lambda p: p1(p).start())

    lane = lax.broadcasted_iota(jnp.int32, (ch, n), 1)

    def spread(c):
        cf[pl.ds(pl.multiple_of(c * stride, 8), n), :] = cot[c].astype(f32)
    loop(ch, spread)

    def pack_edges(g):
        a = jnp.zeros((ch, n), bf)
        b = jnp.zeros((ch, n), bf)
        for s in range(per):
            i = g * per + s
            x = cf[pl.ds(i, ch, stride=stride), :].astype(bf)
            ct[m + i] = x
            here = lane // width == s
            a = jnp.where(here, pltpu.roll(x, width * s, 1) if s else x, a)
            sh = (width * (s + 1)) % n
            b = jnp.where(here, pltpu.roll(x, sh, 1) if sh else x, b)
        edge_l[g] = a
        edge_r[g] = b
    loop(tiles, pack_edges)

    def halos(act):
        last = tiles - 1
        plan = (
            (left, edge_l, from_r.at[pl.ds(1, tiles)], 0, 0, -1),
            (right, edge_r, from_l.at[pl.ds(1, tiles)], 1, 0, 1),
            (above, ct.at[pl.ds(m, m)], bottom, 2, -1, 0),
            (below, ct.at[pl.ds(n, m)], top, 3, 1, 0),
            (below & left, edge_l.at[last], from_r.at[0], 4, 1, -1),
            (above & left, edge_l.at[0], from_r.at[tiles + 1], 5, -1, -1),
            (below & right, edge_r.at[last], from_l.at[0], 6, 1, 1),
            (above & right, edge_r.at[0], from_l.at[tiles + 1], 7, -1, 1),
        )
        flags = {(0, -1): right, (0, 1): left, (-1, 0): below, (1, 0): above,
                 (1, -1): above & right, (-1, -1): below & right, (1, 1): above & left, (-1, 1): below & left}
        for ok, src, dst, k, dq, dt in plan:
            act(ok, flags[(dq, dt)], src, dst, send(src, dst, hs.at[k], hr.at[k], q + dq, t + dt))

    def start(ok, got, src, dst, c):
        @pl.when(ok)
        def _():
            c.start()
    halos(start)

    for s in range(per):
        p = lax.broadcasted_iota(jnp.int32, (2 * n, n), 0)
        x = lax.broadcasted_iota(jnp.int32, (2 * n, n), 1)
        pick = ((p == width * s + x) & (x < width)) | ((p == width * s + x + width) & (x >= n - width) & (p >= n))
        um[:, s * n : (s + 1) * n] = jnp.where(pick, 1.0, 0.0).astype(bf)

    for a in range(3):
        zrow, drow = [None] * 5, [None] * 5
        for b in range(3):
            x = kf[3 * a + b].astype(f32)
            zrow[b - a + 2] = x
            drow[a - b + 2] = x.T
        blank = jnp.zeros((ch, ch), f32)
        fill = lambda xs: jnp.concatenate([blank if x is None else x for x in xs], axis=1).astype(bf)
        wz[a * ch : (a + 1) * ch, :] = fill(zrow)
        wd[a * ch : (a + 1) * ch, :] = fill(drow)

    peers(lambda p: send(pack, blocks.at[p + 1], ps.at[p], pr.at[p], q, t).wait_recv())

    d0 = t * n
    v0 = 2 * ch
    for k in range(4):
        x = blocks[q + t + k].astype(f32)
        cw[k, 0:ch] = x[0:ch]
        cw[k, ch : ch + RG] = x[v0 : v0 + RG]
    hrows = ch + 16
    slots = tiles + 2
    lane_h = lax.broadcasted_iota(jnp.int32, (hrows, n), 1)
    cblk = [jnp.concatenate([blocks[q + t + k, 0:ch], blocks[q + t + k, v0 : v0 + 16]], axis=0) for k in range(4)]
    rblk = [jnp.concatenate([blocks[q + k, ch : 2 * ch], blocks[q + k, v0 : v0 + 16]], axis=0) for k in range(3)]

    for k in range(3):
        rb[k] = rblk[k]

    def window(blks, base):
        k, sh = base // n, base % n
        x = blks[k]
        if sh:
            if k + 1 < len(blks):
                x = jnp.where(lane_h >= sh, x, blks[k + 1])
            x = pltpu.roll(x, n - sh, 1)
        return x
    for g in range(slots):
        for side, off in ((0, 2 * n - per), (1, n - per - width)):
            hlc[(2 * g + side) * hrows : (2 * g + side + 1) * hrows, :] = window(cblk, per * g + off)
        hlr[g * hrows : (g + 1) * hrows, :] = window(rblk, per * g + n - per)
    src = lax.broadcasted_iota(jnp.int32, (n, n), 0)
    dst = lax.broadcasted_iota(jnp.int32, (n, n), 1)
    one = lambda cond: jnp.where(cond, 1.0, 0.0).astype(bf)
    hc = jnp.dot(hlc[...], one(src == dst // width + dst % width), preferred_element_type=f32)
    hw = jnp.dot(hlr[...], one(src == dst // width), preferred_element_type=f32)
    kk = lax.broadcasted_iota(jnp.int32, (RG, n), 1) % width
    for g in range(slots):
        hrw = hw[g * hrows : (g + 1) * hrows]
        for side in range(2):
            hcc = hc[(2 * g + side) * hrows : (2 * g + side + 1) * hrows]
            da = d0 + kk + (-width if side else n)
            v8 = jnp.where((da >= 0) & (da < w), hcc[ch : ch + RG] * hrw[ch : ch + RG], 0.0)
            v = jnp.concatenate([v8] * (ch // RG), axis=0)
            hh[side, g] = (hrw[0:ch] + hcc[0:ch]) * v
            hval[side, g] = jnp.concatenate([v8, v8], axis=0).astype(bf)

    lane8 = lax.broadcasted_iota(jnp.int32, (RG, n), 1)
    lane40 = lax.broadcasted_iota(jnp.int32, (ch + RG, n), 1)
    lane16 = lax.broadcasted_iota(jnp.int32, (16, n), 1)
    sub16 = lax.broadcasted_iota(jnp.int32, (16, n), 0)

    def unpack(dst):
        for j in range(per // 2):
            y = jnp.dot(hpk[...], um[:, 2 * j * n : 2 * (j + 1) * n], preferred_element_type=f32)
            for g in range(slots):
                for s in range(2):
                    dst[g * per + 2 * j + s] = y[g * ch : (g + 1) * ch, s * n : (s + 1) * n].astype(bf)
    def shifts(dst, halo, gi):
        for ii in range(RG):
            e = gi * RG + ii
            hx, main = halo[e + per - m], dst[e, 2 * ch : 3 * ch]
            for k in (1, 2):
                sr = k * r
                dst[e, (2 + k) * ch : (3 + k) * ch] = pltpu.roll(jnp.where(lane < sr, hx, main), n - sr, 1)
                dst[e, (2 - k) * ch : (3 - k) * ch] = pltpu.roll(jnp.where(lane >= n - sr, hx, main), sr, 1)

    ones = jnp.ones((n, n), bf)

    def prep(gi):
        picks, vrow, where_at = [], jnp.zeros((16, n), bf), []
        for ii in range(RG):
            at = gi * RG + ii - m + n
            k, sh = at // n, lax.rem(at, n)
            where_at.append((k, sh))
            x = rb[k]
            picks.append(jnp.where(lane == sh, x[:ch], 0.0))
            vrow = jnp.where((sub16 == ii) & (lane16 == sh), x[ch:], vrow)
        rw = jnp.dot(jnp.concatenate(picks + [vrow], axis=0), ones, preferred_element_type=f32)
        for ii in range(RG):
            e = gi * RG + ii
            k, sh = where_at[ii]
            c = pltpu.roll(jnp.where(lane40 >= sh, cw[k], cw[k + 1]), (n - sh) & (n - 1), 1)
            vr = rw[RG * ch + ii : RG * ch + ii + 1]
            v8 = jnp.where(lane8 + d0 < w, c[ch:] * vr, 0.0)
            vb[e] = v8
            x = jnp.concatenate([v8, v8], axis=0).astype(bf)
            vb16[e] = x
            hid[e] = (rw[ii * ch : (ii + 1) * ch] + c[:ch]) * jnp.concatenate([v8] * (ch // RG), axis=0)
            gz5[e, 2 * ch : 3 * ch] = ct[e] * jnp.concatenate([x, x], axis=0)

    def gelus(gi):
        for ii in range(RG):
            e = gi * RG + ii
            h = hid[e]
            h2 = h * h
            cdf = 0.5 + 0.5 * jnp.tanh(h * (S2PI + (S2PI * CUBIC) * h2))
            act = (h * cdf).astype(bf)
            act5[e, 2 * ch : 3 * ch] = act
            actm[e + m] = act
            x = h * (2.0 * S2PI + (6.0 * S2PI * CUBIC) * h2)
            cv = cdf * jnp.concatenate([vb[e]] * (ch // RG), axis=0)
            der[e] = cv + cv * ((1.0 - cdf) * x)

    def kgrad(gi):
        xs, gs = [], []
        for ii in range(RG):
            e = gi * RG + ii
            gs.append(gz5[e])
            xs.append(jnp.concatenate([actm[e + m + (a - 1) * r] for a in range(3)], axis=0))
        kacc[...] += lax.dot_general(jnp.concatenate(gs, axis=1), jnp.concatenate(xs, axis=1),
                                     (((1,), (1,)), ((), ())), preferred_element_type=f32)

    def pipeline(stages, counts, lags):
        first_full = max(lags)
        last_full = min(c + l for c, l in zip(counts, lags))
        total = max(c + l for c, l in zip(counts, lags))

        def at_step(j):
            for f, c, l in zip(stages, counts, lags):
                if 0 <= j - l < c:
                    f(j - l)
        for j in range(first_full):
            at_step(j)

        def body(j):
            for f, l in zip(stages, lags):
                f(j + first_full - l)
        loop(last_full - first_full, body)
        for j in range(last_full, total):
            at_step(j)

    ge, gm = ext // RG, n // RG
    kacc[...] = jnp.zeros_like(kacc)
    for e in range(m):
        ct[e] = jnp.zeros((ch, n), bf)
        ct[n + m + e] = jnp.zeros((ch, n), bf)
    pipeline((gelus, prep), (ge,) * 2, (1, 0))
    for e in range(2 * m):
        actm[e] = jnp.zeros((ch, n), bf)
        actm[n + 2 * m + e] = jnp.zeros((ch, n), bf)

    def bsums(gi, tot):
        for ii in range(2 * RG):
            tot = tot + gz5[m + gi * 2 * RG + ii, 2 * ch : 3 * ch].astype(f32)
        return tot
    btot = lax.fori_loop(0, n // (2 * RG), bsums, jnp.zeros((ch, n), f32))

    def finish(ok, got, src, dst, c):
        @pl.when(got)
        def _():
            c.wait_recv()

        @pl.when(jnp.logical_not(got))
        def _():
            dst[...] = jnp.zeros(dst.shape, bf)
    halos(finish)

    for g in range(slots):
        for side, buf in ((0, from_r), (1, from_l)):
            x = hval[side, g]
            hpk[g * ch : (g + 1) * ch, side * n : (side + 1) * n] = buf[g] * jnp.concatenate([x, x], axis=0)
    unpack(hg)
    for e in range(m):
        for buf, at in ((top, e), (bottom, n + m + e)):
            x = vb16[at]
            gz5[at, 2 * ch : 3 * ch] = buf[e] * jnp.concatenate([x, x], axis=0)

    def conv_d(gi):
        y = jnp.dot(wd[...], jnp.concatenate([gz5[gi * RG + ii] for ii in range(RG)], axis=1), preferred_element_type=f32)
        for ii in range(RG):
            yd[gi * RG + ii] = y[:, ii * n : (ii + 1) * n]

    csum[...] = jnp.zeros_like(csum)

    def backward(gi):
        lo, hi = csum[0], csum[1]
        for ii in range(RG):
            i = gi * RG + ii
            da = yd[m + i + r, 0:ch] + yd[m + i, ch : 2 * ch] + yd[m + i - r, 2 * ch : 3 * ch]
            dx = gz5[m + i, 2 * ch : 3 * ch].astype(f32) + der[m + i] * da
            der[m + i] = dx
            x = pltpu.roll(dx, i, 1)
            wrap = lane < i
            lo = lo + jnp.where(wrap, 0.0, x)
            hi = hi + jnp.where(wrap, x, 0.0)
        csum[0] = lo
        csum[1] = hi
    pipeline((backward, kgrad, conv_d, lambda g: shifts(gz5, hg, g)), (gm, ge, ge, ge), (3, 1, 1, 0))
    for a in range(3):
        for b in range(3):
            k = a - b + 2
            x = kacc[k * ch : (k + 1) * ch, a * ch : (a + 1) * ch]
            kg[3 * a + b] = jnp.concatenate([x[z * RG : (z + 1) * RG] for z in range(ch // RG)], axis=1)
    diag = lax.broadcasted_iota(jnp.int32, (ch, n), 0) == lane
    bt = jnp.sum(btot, axis=1, keepdims=True)
    kg[9] = jnp.broadcast_to(jnp.sum(jnp.where(diag, bt, 0.0), axis=0, keepdims=True), (RG, n))

    def k1(k):
        return send(kg.at[k], kbuf.at[me], ks.at[k], kr.at[me], k // T, k % T)

    def first_k(act):
        for k in range(K):
            @pl.when(me != k)
            def _():
                act(k1(k))
    first_k(lambda c: c.start())

    lo, hi = csum[0], csum[1]

    def row_sums(gi, rsum):
        for ii in range(2 * RG):
            i = gi * 2 * RG + ii
            rsum = jnp.where(lane == i, jnp.sum(der[m + i], axis=1, keepdims=True), rsum)
        return rsum
    rsum = lax.fori_loop(0, n // (2 * RG), row_sums, jnp.zeros((ch, n), f32))
    for z in range(Z):
        sl = slice(z * RG, (z + 1) * RG)
        row[z] = rsum[sl]
        col[0, z] = lo[sl]
        col[1, z] = hi[sl]

    def root(z):
        return (T - 2) // 2 + z % 2 if T > 1 else 0

    def r1(z):
        return send(row.at[z], rbuf.at[z, t], rs.at[z], rr.at[z, t], q, root(z))

    def a1(z):
        return send(col.at[0, z], abuf.at[z, q], as_.at[z], ar.at[z, q], q + t, root(z))

    def b1(z):
        return send(col.at[1, z], bbuf.at[z, q], bs.at[z], br.at[z, q], q + t + 1, root(z))

    def first(act):
        for z in range(Z):
            @pl.when(t != root(z))
            def _():
                act(r1(z))

            @pl.when((q + t < R) & ((t != 0) | (root(z) != 0)))
            def _():
                act(a1(z))

            @pl.when(q + t + 1 < R)
            def _():
                act(b1(z))

    first(lambda c: c.start())

    for g in range(slots):
        for side in range(2):
            h = hh[side, g]
            _, _, cdf = gelu_parts(h)
            hpk[g * ch : (g + 1) * ch, side * n : (side + 1) * n] = (h * cdf).astype(bf)
    unpack(ha)
    loop(ge, lambda g: shifts(act5, ha, g))

    gr = divisor(ext, 34)

    def conv_z(gi):
        y = jnp.dot(wz[...], jnp.concatenate([act5[gi * gr + ii] for ii in range(gr)], axis=1), preferred_element_type=f32)
        for ii in range(gr):
            yz[gi * gr + ii] = y[:, ii * n : (ii + 1) * n]

    def got(buf, sem):
        send(buf, buf, sem, sem, q, t).wait_recv()

    def k2(p):
        return send(ksum, kres.at[me], k2s.at[p], k2r.at[me], p // T, p % T)

    def second_k(act):
        @pl.when(me < K)
        def _():
            def one(p):
                @pl.when(p != me)
                def _():
                    act(k2(p))
            loop(N, one)

    def r2(z, p):
        return send(rcsum.at[z], rcres.at[z], r2s.at[z, p], r2r.at[z], q, p)

    def second(act):
        for z in range(Z):
            @pl.when(t == root(z))
            def _():
                def one(p):
                    @pl.when(p != t)
                    def _():
                        act(r2(z, p))
                loop(T, one)

    for z in range(Z):
        @pl.when(t == root(z))
        def _():
            rcsum[z, 0] = row[z]
            rcsum[z, 1] = jnp.zeros((RG, n), f32)

            def take(p):
                @pl.when(p != t)
                def _():
                    got(rbuf.at[z, p], rr.at[z, p])
                    rcsum[z, 0] += rbuf[z, p]
            loop(T, take)

            @pl.when(t == 0)
            def _():
                rcsum[z, 1] = col[0, z]

            def take_col(p):
                @pl.when((p <= q) & (q - p < T) & ((p != q) | (t != 0)))
                def _():
                    got(abuf.at[z, p], ar.at[z, p])
                    rcsum[z, 1] += abuf[z, p]

                @pl.when((p <= q - 1) & (q - 1 - p < T))
                def _():
                    got(bbuf.at[z, p], br.at[z, p])
                    rcsum[z, 1] += bbuf[z, p]
            loop(R, take_col)
            rcsum[z] = rcsum[z] * embed_scale
            rcres[z] = rcsum[z]
    second(lambda c: c.start())

    @pl.when(me < K)
    def _():
        ksum[...] = kg[me]

        def take(p):
            @pl.when(p != me)
            def _():
                got(kbuf.at[p], kr.at[p])
                ksum[...] += kbuf[p]
        loop(N, take)
        ksum[...] = ksum[...] * weight_scale
        kres[me] = ksum[...]
    second_k(lambda c: c.start())
    loop(ext // gr, conv_z)

    eye = lax.broadcasted_iota(jnp.int32, (ch, ch), 0) == lax.broadcasted_iota(jnp.int32, (ch, ch), 1)
    bcol = jnp.sum(jnp.where(eye, bias[...], 0.0), axis=1, keepdims=True)
    bias_all = jnp.broadcast_to(bcol, (ch, n))

    def phase_o(gi):
        for ii in range(RG):
            i = gi * RG + ii
            z = yz[m + i - r, 0:ch] + yz[m + i, ch : 2 * ch] + yz[m + i + r, 2 * ch : 3 * ch]
            v = jnp.concatenate([vb[m + i]] * (ch // RG), axis=0)
            cf[pl.ds(i, ch, stride=stride), :] = (hid[m + i] + z + bias_all) * v
    loop(gm, phase_o)

    def emit(c):
        out[c] = cf[pl.ds(pl.multiple_of(c * stride, 8), n), :].astype(bf)
    loop(ch, emit)

    for k in range(K):
        @pl.when(me != k)
        def _():
            got(kres.at[k], k2r.at[k])
    for z in range(Z):
        @pl.when(t != root(z))
        def _():
            got(rcres.at[z], r2r.at[z])
    peers(lambda p: p1(p).wait_send())

    def sent(ok, got, src, dst, c):
        @pl.when(ok)
        def _():
            c.wait_send()
    halos(sent)
    first_k(lambda c: c.wait_send())
    first(lambda c: c.wait_send())
    second_k(lambda c: c.wait_send())
    second(lambda c: c.wait_send())


def finish_kernel(pair, kres, rcres, out, row_out, col_out, kg_out, bg_out):
    out[...] = pair[...]
    ch = row_out.shape[0]
    for z in range(ch // RG):
        row_out[z * RG : (z + 1) * RG, :] = rcres[z, 0]
        col_out[z * RG : (z + 1) * RG, :] = rcres[z, 1]
        for s in range(9):
            kg_out[s, z * RG : (z + 1) * RG, :] = kres[s, :, z * ch : (z + 1) * ch]
    bg_out[...] = kres[9, 0:1, 0:ch]


def local(emb_rows, emb_cols, kernel, bias, cotangent, valid, dilation, band):
    ch, n = emb_rows.shape
    R, T = lax.axis_size("row"), lax.axis_size("diag")
    m = MAXDIL
    ext = n + 2 * m
    vmem = pl.BlockSpec(memory_space=pltpu.VMEM)
    smem = pl.BlockSpec(memory_space=pltpu.SMEM)
    dma = pltpu.SemaphoreType.DMA
    V = pltpu.VMEM
    width = 2 * m
    per = n // width
    tiles = n // per
    slots = tiles + 2
    hrows = ch + 16
    kf = kernel.reshape(9, ch, ch)
    nk = (9 * ch * ch) // (RG * 128) + 1
    Z = ch // RG
    tile = lambda *lead: V(lead + (RG, n), f32)
    edges = lambda k: V((k, ch, n), bf)
    embed_scale = float(T * n) ** -0.5
    weight_scale = float(R * n * T * n) ** -0.5
    pair, kres, rcres = pl.pallas_call(
        functools.partial(fused_kernel, R, T, embed_scale, weight_scale),
        out_shape=(
            V((ch, n, n), bf),
            V((nk, RG, n), f32),
            V((Z, 2, RG, n), f32),
        ),
        in_specs=[smem, smem] + [vmem] * 6,
        out_specs=(vmem,) * 3,
        scratch_shapes=[
            V((2 * ch + 16, n), bf), V((R + T + 3, 2 * ch + 16, n), bf), V((ch * (n + 8), n), f32),
            edges(ext), edges(tiles), edges(tiles), edges(slots), edges(slots), edges(m), edges(m),
            V((4, ch + RG, n), f32), V((3, ch + 16, n), bf),
            V((slots * 2 * hrows, n), bf), V((slots * hrows, n), bf),
            V((slots * ch, 2 * n), bf), V((2, slots, 16, n), bf), V((2 * n, per * n), bf), edges(slots * per), edges(slots * per),
            V((ext, 5 * ch, n), bf), V((ext, 5 * ch, n), bf), V((ext + 2 * m, ch, n), bf), V((2, slots, ch, n), f32),
            V((ext, ch, n), f32), V((ext, ch, n), f32), V((ext, RG, n), f32), V((ext, 16, n), bf),
            V((ext, 3 * ch, n), f32), V((ext, 3 * ch, n), f32),
            V((3 * ch, 5 * ch), bf), V((3 * ch, 5 * ch), bf), V((5 * ch, 3 * ch), f32),
            V((2, ch, n), f32), tile(nk), tile(Z), tile(2, Z),
            tile(R * T), tile(Z, T), tile(Z, R), tile(Z, R), tile(), tile(Z, 2),
            dma((R,)), dma((R,)), dma((8,)), dma((8,)),
            dma((nk,)), dma((R * T,)), dma((Z,)), dma((Z, T)), dma((Z,)), dma((Z, R)), dma((Z,)), dma((Z, R)),
            dma((R * T,)), dma((nk,)), dma((Z, T)), dma((Z,)),
        ],
        compiler_params=pltpu.CompilerParams(collective_id=0, has_side_effects=True, vmem_limit_bytes=56 * 2**20),
        name="fused_kernel",
    )(dilation, band, emb_rows, emb_cols, valid[None, :], kf, bias[None, :], cotangent)

    out, row_grad, col_grad, kgt, bgt = pl.pallas_call(
        finish_kernel,
        out_shape=(
            jax.ShapeDtypeStruct((ch, n, n), bf),
            jax.ShapeDtypeStruct((ch, n), f32),
            jax.ShapeDtypeStruct((ch, n), f32),
            jax.ShapeDtypeStruct((9, ch, ch), f32),
            jax.ShapeDtypeStruct((1, ch), f32),
        ),
        in_specs=[vmem] * 3,
        out_specs=(vmem,) * 5,
        name="finish_kernel",
    )(*(pltpu.with_memory_space_constraint(x, V) for x in (pair, kres, rcres)))
    return out, row_grad, col_grad, kgt.reshape(3, 3, ch, ch), bgt.reshape(ch)


def solution(mesh):
    in_specs = (
        P(None, ("grp", "row")),
        P(None, ("grp", "row")),
        P(),
        P(),
        P(None, ("grp", "row"), "diag"),
        P(("grp", "row")),
        P("grp"),
        P("grp"),
    )
    out_specs = (
        P(None, ("grp", "row"), "diag"),
        P(None, ("grp", "row")),
        P(None, ("grp", "row")),
        P("grp", None, None, None),
        P("grp"),
    )
    return jax.shard_map(local, mesh=mesh, in_specs=in_specs, out_specs=out_specs, check_vma=False)
```

```python
import functools

import jax
import jax.numpy as jnp
from jax import lax
from jax.experimental import pallas as pl
from jax.experimental.pallas import tpu as pltpu
from jax.sharding import PartitionSpec as P

MAXDIL = 4
RG = 8
S2PI = 0.7978845608028654
CUBIC = 0.044715
bf, f32 = jnp.bfloat16, jnp.float32


def loop(count, body):
    def step(p, c):
        body(p)
        return c
    lax.fori_loop(0, count, step, 0)


def send(src, dst, ss, sr, dq, dt):
    return pltpu.make_async_remote_copy(
        src_ref=src, dst_ref=dst, send_sem=ss, recv_sem=sr,
        device_id={"row": dq, "diag": dt}, device_id_type=pl.DeviceIdType.MESH,
    )


def gelu_parts(h):
    h2 = h * h
    t = jnp.tanh(h * (S2PI + (S2PI * CUBIC) * h2))
    cdf = 0.5 + 0.5 * t
    return h2, t, cdf


def divisor(total, limit):
    return max(k for k in range(1, limit + 1) if total % k == 0)


def fused_kernel(
    R, T, embed_scale, weight_scale,
    dilation, band, rows, cols, valid, kf, bias, cot_hbm,
    out, kres, rcres,
    pack, blocks, cf, ct, edge_l, edge_r, from_r, from_l, top, bottom,
    cw, rb, hlc, hlr, hpk, hval, um, ha, hg,
    act5, gz5, actm, hh, hid, der, vb, vb16, yz, yd, wz, wd, kacc, csum, kg, row, col,
    kbuf, rbuf, abuf, bbuf, ksum, rcsum,
    cot, cs, ps, pr, hs, hr, ks, kr, rs, rr, as_, ar, bs, br, k2s, k2r, r2s, r2r,
):
    ch, n = rows.shape
    m = MAXDIL
    width = 2 * m
    per = n // width
    tiles = n // per
    ext = n + 2 * m
    stride = cf.shape[0] // ch
    N = R * T
    K, Z = kg.shape[0], row.shape[0]
    q, t = lax.axis_index("row"), lax.axis_index("diag")
    me = q * T + t
    r, w = dilation[0], band[0]
    mesh_id = pl.DeviceIdType.MESH
    load = pltpu.make_async_copy(cot_hbm, cot, cs)
    load.start()
    barrier = pltpu.get_barrier_semaphore()
    left, right, above, below = t > 0, t < T - 1, q > 0, q < R - 1

    def greet(p):
        @pl.when(p != me)
        def _():
            pl.semaphore_signal(barrier, inc=1, device_id={"row": p // T, "diag": p % T}, device_id_type=mesh_id)
    loop(N, greet)

    pack[0:ch] = cols[...]
    pack[ch : 2 * ch] = rows[...]
    pack[2 * ch : 2 * ch + 16] = jnp.broadcast_to(valid[...].astype(f32), (16, n)).astype(bf)
    zero = jnp.zeros(pack.shape, bf)
    blocks[0] = zero
    for k in range(R + 1, R + T + 3):
        blocks[k] = zero
    blocks[q + 1] = pack[...]
    pl.semaphore_wait(barrier, N - 1)

    def p1(p):
        return send(pack, blocks.at[q + 1], ps.at[p], pr.at[q], p, t)

    def peers(act):
        def one(p):
            @pl.when(p != q)
            def _():
                act(p)
        loop(R, one)
    peers(lambda p: p1(p).start())

    lane = lax.broadcasted_iota(jnp.int32, (ch, n), 1)

    def spread(c):
        cf[pl.ds(pl.multiple_of(c * stride, 8), n), :] = cot[c].astype(f32)
    load.wait()
    loop(ch, spread)

    def pack_edges(g):
        a = jnp.zeros((ch, n), bf)
        b = jnp.zeros((ch, n), bf)
        for s in range(per):
            i = g * per + s
            x = cf[pl.ds(i, ch, stride=stride), :].astype(bf)
            ct[m + i] = x
            here = lane // width == s
            a = jnp.where(here, pltpu.roll(x, width * s, 1) if s else x, a)
            sh = (width * (s + 1)) % n
            b = jnp.where(here, pltpu.roll(x, sh, 1) if sh else x, b)
        edge_l[g] = a
        edge_r[g] = b
    loop(tiles, pack_edges)

    def halos(act):
        last = tiles - 1
        plan = (
            (left, edge_l, from_r.at[pl.ds(1, tiles)], 0, 0, -1),
            (right, edge_r, from_l.at[pl.ds(1, tiles)], 1, 0, 1),
            (above, ct.at[pl.ds(m, m)], bottom, 2, -1, 0),
            (below, ct.at[pl.ds(n, m)], top, 3, 1, 0),
            (below & left, edge_l.at[last], from_r.at[0], 4, 1, -1),
            (above & left, edge_l.at[0], from_r.at[tiles + 1], 5, -1, -1),
            (below & right, edge_r.at[last], from_l.at[0], 6, 1, 1),
            (above & right, edge_r.at[0], from_l.at[tiles + 1], 7, -1, 1),
        )
        flags = {(0, -1): right, (0, 1): left, (-1, 0): below, (1, 0): above,
                 (1, -1): above & right, (-1, -1): below & right, (1, 1): above & left, (-1, 1): below & left}
        for ok, src, dst, k, dq, dt in plan:
            act(ok, flags[(dq, dt)], src, dst, send(src, dst, hs.at[k], hr.at[k], q + dq, t + dt))

    def start(ok, got, src, dst, c):
        @pl.when(ok)
        def _():
            c.start()
    halos(start)

    for s in range(per):
        p = lax.broadcasted_iota(jnp.int32, (2 * n, n), 0)
        x = lax.broadcasted_iota(jnp.int32, (2 * n, n), 1)
        pick = ((p == width * s + x) & (x < width)) | ((p == width * s + x + width) & (x >= n - width) & (p >= n))
        um[:, s * n : (s + 1) * n] = jnp.where(pick, 1.0, 0.0).astype(bf)

    for a in range(3):
        zrow, drow = [None] * 5, [None] * 5
        for b in range(3):
            x = kf[3 * a + b].astype(f32)
            zrow[b - a + 2] = x
            drow[a - b + 2] = x.T
        blank = jnp.zeros((ch, ch), f32)
        fill = lambda xs: jnp.concatenate([blank if x is None else x for x in xs], axis=1).astype(bf)
        wz[a * ch : (a + 1) * ch, :] = fill(zrow)
        wd[a * ch : (a + 1) * ch, :] = fill(drow)

    peers(lambda p: send(pack, blocks.at[p + 1], ps.at[p], pr.at[p], q, t).wait_recv())

    d0 = t * n
    v0 = 2 * ch
    for k in range(4):
        x = blocks[q + t + k].astype(f32)
        cw[k, 0:ch] = x[0:ch]
        cw[k, ch : ch + RG] = x[v0 : v0 + RG]
    hrows = ch + 16
    slots = tiles + 2
    lane_h = lax.broadcasted_iota(jnp.int32, (hrows, n), 1)
    cblk = [jnp.concatenate([blocks[q + t + k, 0:ch], blocks[q + t + k, v0 : v0 + 16]], axis=0) for k in range(4)]
    rblk = [jnp.concatenate([blocks[q + k, ch : 2 * ch], blocks[q + k, v0 : v0 + 16]], axis=0) for k in range(3)]

    for k in range(3):
        rb[k] = rblk[k]

    def window(blks, base):
        k, sh = base // n, base % n
        x = blks[k]
        if sh:
            if k + 1 < len(blks):
                x = jnp.where(lane_h >= sh, x, blks[k + 1])
            x = pltpu.roll(x, n - sh, 1)
        return x
    for g in range(slots):
        for side, off in ((0, 2 * n - per), (1, n - per - width)):
            hlc[(2 * g + side) * hrows : (2 * g + side + 1) * hrows, :] = window(cblk, per * g + off)
        hlr[g * hrows : (g + 1) * hrows, :] = window(rblk, per * g + n - per)
    src = lax.broadcasted_iota(jnp.int32, (n, n), 0)
    dst = lax.broadcasted_iota(jnp.int32, (n, n), 1)
    one = lambda cond: jnp.where(cond, 1.0, 0.0).astype(bf)
    hc = jnp.dot(hlc[...], one(src == dst // width + dst % width), preferred_element_type=f32)
    hw = jnp.dot(hlr[...], one(src == dst // width), preferred_element_type=f32)
    kk = lax.broadcasted_iota(jnp.int32, (RG, n), 1) % width
    for g in range(slots):
        hrw = hw[g * hrows : (g + 1) * hrows]
        for side in range(2):
            hcc = hc[(2 * g + side) * hrows : (2 * g + side + 1) * hrows]
            da = d0 + kk + (-width if side else n)
            v8 = jnp.where((da >= 0) & (da < w), hcc[ch : ch + RG] * hrw[ch : ch + RG], 0.0)
            v = jnp.concatenate([v8] * (ch // RG), axis=0)
            hh[side, g] = (hrw[0:ch] + hcc[0:ch]) * v
            hval[side, g] = jnp.concatenate([v8, v8], axis=0).astype(bf)

    lane8 = lax.broadcasted_iota(jnp.int32, (RG, n), 1)
    lane40 = lax.broadcasted_iota(jnp.int32, (ch + RG, n), 1)
    lane16 = lax.broadcasted_iota(jnp.int32, (16, n), 1)
    sub16 = lax.broadcasted_iota(jnp.int32, (16, n), 0)

    def unpack(dst):
        for j in range(per // 2):
            y = jnp.dot(hpk[...], um[:, 2 * j * n : 2 * (j + 1) * n], preferred_element_type=f32)
            for g in range(slots):
                for s in range(2):
                    dst[g * per + 2 * j + s] = y[g * ch : (g + 1) * ch, s * n : (s + 1) * n].astype(bf)
    def shifts(dst, halo, gi):
        for ii in range(RG):
            e = gi * RG + ii
            hx, main = halo[e + per - m], dst[e, 2 * ch : 3 * ch]
            for k in (1, 2):
                sr = k * r
                dst[e, (2 + k) * ch : (3 + k) * ch] = pltpu.roll(jnp.where(lane < sr, hx, main), n - sr, 1)
                dst[e, (2 - k) * ch : (3 - k) * ch] = pltpu.roll(jnp.where(lane >= n - sr, hx, main), sr, 1)

    ones = jnp.ones((n, n), bf)

    def prep(gi):
        picks, vrow, where_at = [], jnp.zeros((16, n), bf), []
        for ii in range(RG):
            at = gi * RG + ii - m + n
            k, sh = at // n, lax.rem(at, n)
            where_at.append((k, sh))
            x = rb[k]
            picks.append(jnp.where(lane == sh, x[:ch], 0.0))
            vrow = jnp.where((sub16 == ii) & (lane16 == sh), x[ch:], vrow)
        rw = jnp.dot(jnp.concatenate(picks + [vrow], axis=0), ones, preferred_element_type=f32)
        for ii in range(RG):
            e = gi * RG + ii
            k, sh = where_at[ii]
            c = pltpu.roll(jnp.where(lane40 >= sh, cw[k], cw[k + 1]), (n - sh) & (n - 1), 1)
            vr = rw[RG * ch + ii : RG * ch + ii + 1]
            v8 = jnp.where(lane8 + d0 < w, c[ch:] * vr, 0.0)
            vb[e] = v8
            x = jnp.concatenate([v8, v8], axis=0).astype(bf)
            vb16[e] = x
            hid[e] = (rw[ii * ch : (ii + 1) * ch] + c[:ch]) * jnp.concatenate([v8] * (ch // RG), axis=0)
            gz5[e, 2 * ch : 3 * ch] = ct[e] * jnp.concatenate([x, x], axis=0)

    def gelus(gi):
        for ii in range(RG):
            e = gi * RG + ii
            h = hid[e]
            h2 = h * h
            cdf = 0.5 + 0.5 * jnp.tanh(h * (S2PI + (S2PI * CUBIC) * h2))
            act = (h * cdf).astype(bf)
            act5[e, 2 * ch : 3 * ch] = act
            actm[e + m] = act
            x = h * (2.0 * S2PI + (6.0 * S2PI * CUBIC) * h2)
            cv = cdf * jnp.concatenate([vb[e]] * (ch // RG), axis=0)
            der[e] = cv + cv * ((1.0 - cdf) * x)

    def kgrad(gi):
        xs, gs = [], []
        for ii in range(RG):
            e = gi * RG + ii
            gs.append(gz5[e])
            xs.append(jnp.concatenate([actm[e + m + (a - 1) * r] for a in range(3)], axis=0))
        kacc[...] += lax.dot_general(jnp.concatenate(gs, axis=1), jnp.concatenate(xs, axis=1),
                                     (((1,), (1,)), ((), ())), preferred_element_type=f32)

    def pipeline(stages, counts, lags):
        first_full = max(lags)
        last_full = min(c + l for c, l in zip(counts, lags))
        total = max(c + l for c, l in zip(counts, lags))

        def at_step(j):
            for f, c, l in zip(stages, counts, lags):
                if 0 <= j - l < c:
                    f(j - l)
        for j in range(first_full):
            at_step(j)

        def body(j):
            for f, l in zip(stages, lags):
                f(j + first_full - l)
        loop(last_full - first_full, body)
        for j in range(last_full, total):
            at_step(j)

    ge, gm = ext // RG, n // RG
    kacc[...] = jnp.zeros_like(kacc)
    for e in range(m):
        ct[e] = jnp.zeros((ch, n), bf)
        ct[n + m + e] = jnp.zeros((ch, n), bf)
    pipeline((gelus, prep), (ge,) * 2, (1, 0))
    for e in range(2 * m):
        actm[e] = jnp.zeros((ch, n), bf)
        actm[n + 2 * m + e] = jnp.zeros((ch, n), bf)

    def bsums(gi, tot):
        for ii in range(2 * RG):
            tot = tot + gz5[m + gi * 2 * RG + ii, 2 * ch : 3 * ch].astype(f32)
        return tot
    btot = lax.fori_loop(0, n // (2 * RG), bsums, jnp.zeros((ch, n), f32))

    def finish(ok, got, src, dst, c):
        @pl.when(got)
        def _():
            c.wait_recv()

        @pl.when(jnp.logical_not(got))
        def _():
            dst[...] = jnp.zeros(dst.shape, bf)
    halos(finish)

    for g in range(slots):
        for side, buf in ((0, from_r), (1, from_l)):
            x = hval[side, g]
            hpk[g * ch : (g + 1) * ch, side * n : (side + 1) * n] = buf[g] * jnp.concatenate([x, x], axis=0)
    unpack(hg)
    for e in range(m):
        for buf, at in ((top, e), (bottom, n + m + e)):
            x = vb16[at]
            gz5[at, 2 * ch : 3 * ch] = buf[e] * jnp.concatenate([x, x], axis=0)

    def conv_d(gi):
        y = jnp.dot(wd[...], jnp.concatenate([gz5[gi * RG + ii] for ii in range(RG)], axis=1), preferred_element_type=f32)
        for ii in range(RG):
            yd[gi * RG + ii] = y[:, ii * n : (ii + 1) * n]

    csum[...] = jnp.zeros_like(csum)

    def backward(gi):
        lo, hi = csum[0], csum[1]
        for ii in range(RG):
            i = gi * RG + ii
            da = yd[m + i + r, 0:ch] + yd[m + i, ch : 2 * ch] + yd[m + i - r, 2 * ch : 3 * ch]
            dx = gz5[m + i, 2 * ch : 3 * ch].astype(f32) + der[m + i] * da
            der[m + i] = dx
            x = pltpu.roll(dx, i, 1)
            wrap = lane < i
            lo = lo + jnp.where(wrap, 0.0, x)
            hi = hi + jnp.where(wrap, x, 0.0)
        csum[0] = lo
        csum[1] = hi
    pipeline((backward, kgrad, conv_d, lambda g: shifts(gz5, hg, g)), (gm, ge, ge, ge), (3, 1, 1, 0))
    for a in range(3):
        for b in range(3):
            k = a - b + 2
            x = kacc[k * ch : (k + 1) * ch, a * ch : (a + 1) * ch]
            kg[3 * a + b] = jnp.concatenate([x[z * RG : (z + 1) * RG] for z in range(ch // RG)], axis=1)
    diag = lax.broadcasted_iota(jnp.int32, (ch, n), 0) == lane
    bt = jnp.sum(btot, axis=1, keepdims=True)
    kg[9] = jnp.broadcast_to(jnp.sum(jnp.where(diag, bt, 0.0), axis=0, keepdims=True), (RG, n))

    def k1(k):
        return send(kg.at[k], kbuf.at[me], ks.at[k], kr.at[me], k // T, k % T)

    def first_k(act):
        for k in range(K):
            @pl.when(me != k)
            def _():
                act(k1(k))
    first_k(lambda c: c.start())

    lo, hi = csum[0], csum[1]

    def row_sums(gi, rsum):
        for ii in range(2 * RG):
            i = gi * 2 * RG + ii
            rsum = jnp.where(lane == i, jnp.sum(der[m + i], axis=1, keepdims=True), rsum)
        return rsum
    rsum = lax.fori_loop(0, n // (2 * RG), row_sums, jnp.zeros((ch, n), f32))
    for z in range(Z):
        sl = slice(z * RG, (z + 1) * RG)
        row[z] = rsum[sl]
        col[0, z] = lo[sl]
        col[1, z] = hi[sl]

    def root(z):
        return (T - 2) // 2 + z % 2 if T > 1 else 0

    def r1(z):
        return send(row.at[z], rbuf.at[z, t], rs.at[z], rr.at[z, t], q, root(z))

    def a1(z):
        return send(col.at[0, z], abuf.at[z, q], as_.at[z], ar.at[z, q], q + t, root(z))

    def b1(z):
        return send(col.at[1, z], bbuf.at[z, q], bs.at[z], br.at[z, q], q + t + 1, root(z))

    def first(act):
        for z in range(Z):
            @pl.when(t != root(z))
            def _():
                act(r1(z))

            @pl.when((q + t < R) & ((t != 0) | (root(z) != 0)))
            def _():
                act(a1(z))

            @pl.when(q + t + 1 < R)
            def _():
                act(b1(z))

    first(lambda c: c.start())

    for g in range(slots):
        for side in range(2):
            h = hh[side, g]
            _, _, cdf = gelu_parts(h)
            hpk[g * ch : (g + 1) * ch, side * n : (side + 1) * n] = (h * cdf).astype(bf)
    unpack(ha)
    loop(ge, lambda g: shifts(act5, ha, g))

    gr = divisor(ext, 34)

    def conv_z(gi):
        y = jnp.dot(wz[...], jnp.concatenate([act5[gi * gr + ii] for ii in range(gr)], axis=1), preferred_element_type=f32)
        for ii in range(gr):
            yz[gi * gr + ii] = y[:, ii * n : (ii + 1) * n]

    def got(buf, sem):
        send(buf, buf, sem, sem, q, t).wait_recv()

    def k2(p):
        return send(ksum, kres.at[me], k2s.at[p], k2r.at[me], p // T, p % T)

    def second_k(act):
        @pl.when(me < K)
        def _():
            def one(p):
                @pl.when(p != me)
                def _():
                    act(k2(p))
            loop(N, one)

    def r2(z, p):
        return send(rcsum.at[z], rcres.at[z], r2s.at[z, p], r2r.at[z], q, p)

    def second(act):
        for z in range(Z):
            @pl.when(t == root(z))
            def _():
                def one(p):
                    @pl.when(p != t)
                    def _():
                        act(r2(z, p))
                loop(T, one)

    for z in range(Z):
        @pl.when(t == root(z))
        def _():
            rcsum[z, 0] = row[z]
            rcsum[z, 1] = jnp.zeros((RG, n), f32)

            def take(p):
                @pl.when(p != t)
                def _():
                    got(rbuf.at[z, p], rr.at[z, p])
                    rcsum[z, 0] += rbuf[z, p]
            loop(T, take)

            @pl.when(t == 0)
            def _():
                rcsum[z, 1] = col[0, z]

            def take_col(p):
                @pl.when((p <= q) & (q - p < T) & ((p != q) | (t != 0)))
                def _():
                    got(abuf.at[z, p], ar.at[z, p])
                    rcsum[z, 1] += abuf[z, p]

                @pl.when((p <= q - 1) & (q - 1 - p < T))
                def _():
                    got(bbuf.at[z, p], br.at[z, p])
                    rcsum[z, 1] += bbuf[z, p]
            loop(R, take_col)
            rcsum[z] = rcsum[z] * embed_scale
            rcres[z] = rcsum[z]
    second(lambda c: c.start())

    @pl.when(me < K)
    def _():
        ksum[...] = kg[me]

        def take(p):
            @pl.when(p != me)
            def _():
                got(kbuf.at[p], kr.at[p])
                ksum[...] += kbuf[p]
        loop(N, take)
        ksum[...] = ksum[...] * weight_scale
        kres[me] = ksum[...]
    second_k(lambda c: c.start())
    loop(ext // gr, conv_z)

    eye = lax.broadcasted_iota(jnp.int32, (ch, ch), 0) == lax.broadcasted_iota(jnp.int32, (ch, ch), 1)
    bcol = jnp.sum(jnp.where(eye, bias[...], 0.0), axis=1, keepdims=True)
    bias_all = jnp.broadcast_to(bcol, (ch, n))

    def phase_o(gi):
        for ii in range(RG):
            i = gi * RG + ii
            z = yz[m + i - r, 0:ch] + yz[m + i, ch : 2 * ch] + yz[m + i + r, 2 * ch : 3 * ch]
            v = jnp.concatenate([vb[m + i]] * (ch // RG), axis=0)
            cf[pl.ds(i, ch, stride=stride), :] = (hid[m + i] + z + bias_all) * v
    loop(gm, phase_o)

    def emit(c):
        out[c] = cf[pl.ds(pl.multiple_of(c * stride, 8), n), :].astype(bf)
    loop(ch, emit)

    for k in range(K):
        @pl.when(me != k)
        def _():
            got(kres.at[k], k2r.at[k])
    for z in range(Z):
        @pl.when(t != root(z))
        def _():
            got(rcres.at[z], r2r.at[z])
    peers(lambda p: p1(p).wait_send())

    def sent(ok, got, src, dst, c):
        @pl.when(ok)
        def _():
            c.wait_send()
    halos(sent)
    first_k(lambda c: c.wait_send())
    first(lambda c: c.wait_send())
    second_k(lambda c: c.wait_send())
    second(lambda c: c.wait_send())


def finish_kernel(pair, kres, rcres, out, row_out, col_out, kg_out, bg_out):
    out[...] = pair[...]
    ch = row_out.shape[0]
    for z in range(ch // RG):
        row_out[z * RG : (z + 1) * RG, :] = rcres[z, 0]
        col_out[z * RG : (z + 1) * RG, :] = rcres[z, 1]
        for s in range(9):
            kg_out[s, z * RG : (z + 1) * RG, :] = kres[s, :, z * ch : (z + 1) * ch]
    bg_out[...] = kres[9, 0:1, 0:ch]


def local(emb_rows, emb_cols, kernel, bias, cotangent, valid, dilation, band):
    ch, n = emb_rows.shape
    R, T = lax.axis_size("row"), lax.axis_size("diag")
    m = MAXDIL
    ext = n + 2 * m
    vmem = pl.BlockSpec(memory_space=pltpu.VMEM)
    smem = pl.BlockSpec(memory_space=pltpu.SMEM)
    dma = pltpu.SemaphoreType.DMA
    V = pltpu.VMEM
    width = 2 * m
    per = n // width
    tiles = n // per
    slots = tiles + 2
    hrows = ch + 16
    kf = kernel.reshape(9, ch, ch)
    nk = (9 * ch * ch) // (RG * 128) + 1
    Z = ch // RG
    tile = lambda *lead: V(lead + (RG, n), f32)
    edges = lambda k: V((k, ch, n), bf)
    embed_scale = float(T * n) ** -0.5
    weight_scale = float(R * n * T * n) ** -0.5
    pair, kres, rcres = pl.pallas_call(
        functools.partial(fused_kernel, R, T, embed_scale, weight_scale),
        out_shape=(
            V((ch, n, n), bf),
            V((nk, RG, n), f32),
            V((Z, 2, RG, n), f32),
        ),
        in_specs=[smem, smem] + [vmem] * 5 + [pl.BlockSpec(memory_space=pl.ANY)],
        out_specs=(vmem,) * 3,
        scratch_shapes=[
            V((2 * ch + 16, n), bf), V((R + T + 3, 2 * ch + 16, n), bf), V((ch * (n + 8), n), f32),
            edges(ext), edges(tiles), edges(tiles), edges(slots), edges(slots), edges(m), edges(m),
            V((4, ch + RG, n), f32), V((3, ch + 16, n), bf),
            V((slots * 2 * hrows, n), bf), V((slots * hrows, n), bf),
            V((slots * ch, 2 * n), bf), V((2, slots, 16, n), bf), V((2 * n, per * n), bf), edges(slots * per), edges(slots * per),
            V((ext, 5 * ch, n), bf), V((ext, 5 * ch, n), bf), V((ext + 2 * m, ch, n), bf), V((2, slots, ch, n), f32),
            V((ext, ch, n), f32), V((ext, ch, n), f32), V((ext, RG, n), f32), V((ext, 16, n), bf),
            V((ext, 3 * ch, n), f32), V((ext, 3 * ch, n), f32),
            V((3 * ch, 5 * ch), bf), V((3 * ch, 5 * ch), bf), V((5 * ch, 3 * ch), f32),
            V((2, ch, n), f32), tile(nk), tile(Z), tile(2, Z),
            tile(R * T), tile(Z, T), tile(Z, R), tile(Z, R), tile(), tile(Z, 2),
            V((ch, n, n), bf), dma, dma((R,)), dma((R,)), dma((8,)), dma((8,)),
            dma((nk,)), dma((R * T,)), dma((Z,)), dma((Z, T)), dma((Z,)), dma((Z, R)), dma((Z,)), dma((Z, R)),
            dma((R * T,)), dma((nk,)), dma((Z, T)), dma((Z,)),
        ],
        compiler_params=pltpu.CompilerParams(collective_id=0, has_side_effects=True, vmem_limit_bytes=56 * 2**20),
        name="fused_kernel",
    )(dilation, band, emb_rows, emb_cols, valid[None, :], kf, bias[None, :], cotangent)

    out, row_grad, col_grad, kgt, bgt = pl.pallas_call(
        finish_kernel,
        out_shape=(
            jax.ShapeDtypeStruct((ch, n, n), bf),
            jax.ShapeDtypeStruct((ch, n), f32),
            jax.ShapeDtypeStruct((ch, n), f32),
            jax.ShapeDtypeStruct((9, ch, ch), f32),
            jax.ShapeDtypeStruct((1, ch), f32),
        ),
        in_specs=[vmem] * 3,
        out_specs=(vmem,) * 5,
        name="finish_kernel",
    )(*(pltpu.with_memory_space_constraint(x, V) for x in (pair, kres, rcres)))
    return out, row_grad, col_grad, kgt.reshape(3, 3, ch, ch), bgt.reshape(ch)


def solution(mesh):
    in_specs = (
        P(None, ("grp", "row")),
        P(None, ("grp", "row")),
        P(),
        P(),
        P(None, ("grp", "row"), "diag"),
        P(("grp", "row")),
        P("grp"),
        P("grp"),
    )
    out_specs = (
        P(None, ("grp", "row"), "diag"),
        P(None, ("grp", "row")),
        P(None, ("grp", "row")),
        P("grp", None, None, None),
        P("grp"),
    )
    return jax.shard_map(local, mesh=mesh, in_specs=in_specs, out_specs=out_specs, check_vma=False)
```
